128 devices in a mesh: dp: 8 (over z_hi, x), section: 4 (over y), tensor: 4 (over z_lo, core).
Axes of the slice: x: 4, y: 4, z: 4 (z_hi: 2, z_lo: 2; z = z_hi * 2 + z_lo), core: 2. Of those that a mesh axis runs over, the one named last changes fastest.
Arguments:
- failed_section: int32 [8], P('dp'), may hold values from 0 to 999
- token_ids: int32 [8, 2048], P('dp'), may hold values from 0 to 100001, as said below
- section_outputs: bfloat16 [8, 4, 2048, 2048], P('dp', 'section', None, 'tensor'), may hold values from -11 to 11
- w_query: float32 [4, 2048, 1024], P('section', 'dp', 'tensor'), may hold values from -1 to 1
- w_key: float32 [4, 2048, 1024], P('section', 'dp', 'tensor'), may hold values from -2 to 2
- w_value: float32 [4, 2048, 1024], P('section', 'dp', 'tensor'), may hold values from -0.125 to 0.125
- w_out: float32 [4, 2048, 1024], P('section', 'dp', 'tensor'), may hold values from -0.75 to 0.75
- m_value: float32 [4, 2048, 1024], P('section', 'dp', 'tensor'), may hold values from -3 to 3
- v_value: float32 [4, 2048, 1024], P('section', 'dp', 'tensor'), may hold values from 0.001 to 1
- m_out: float32 [4, 2048, 1024], P('section', 'dp', 'tensor'), may hold values from -3 to 3
- v_out: float32 [4, 2048, 1024], P('section', 'dp', 'tensor'), may hold values from 0.001 to 1
Outputs:
- restored_query: float32 [8, 4, 2048, 1024], P('dp', 'section', None, 'tensor')
- restored_key: float32 [8, 4, 2048, 1024], P('dp', 'section', None, 'tensor')
- restored_value: float32 [8, 4, 2048, 1024], P('dp', 'section', None, 'tensor')
- restored_out: float32 [8, 4, 2048, 1024], P('dp', 'section', None, 'tensor')
- restored_m_value: float32 [8, 4, 2048, 1024], P('dp', 'section', None, 'tensor')
- restored_v_value: float32 [8, 4, 2048, 1024], P('dp', 'section', None, 'tensor')
- restored_m_out: float32 [8, 4, 2048, 1024], P('dp', 'section', None, 'tensor')
- restored_v_out: float32 [8, 4, 2048, 1024], P('dp', 'section', None, 'tensor')
- attn_update: bfloat16 [8, 4, 2048, 2048], P('dp', 'section', None, 'tensor')
The draws below stay inside these ranges and needn't reach their ends.
Inputs may be any that keep to these rules, and one draw needn't show every extreme that they name: `token_ids`: token ids of each replica's micro-batch; the id 100001 ends a document, the others are ordinary tokens below 100000.
All inputs are finite; a program needn't handle non-finite values.
Results may differ from the reference program's by a relative error of at most 0.0087.
Values may be sent and summed in bfloat16 or wider, within the bound.
A program may use at most 128 MiB of HBM per device.

```python
import math
import jax
import jax.numpy as jnp
from jax import lax

D = 2048
HD = 128
HEADS = 8
TOKENS = 2048
INNER = 1024
REPLICAS = 8
SECTIONS = 4


def draw_token_ids(key, part):
    word_ids = jax.random.randint(jax.random.fold_in(key, 11), (REPLICAS, TOKENS), 0, 100000)
    doc_marks = jax.random.randint(jax.random.fold_in(key, 12), (REPLICAS, TOKENS), 0, max(2, TOKENS // 8))
    return jnp.where(doc_marks == 0, 100001, word_ids).astype(jnp.int32)


def draw_section_outputs(key, part):
    full_shape = (REPLICAS, SECTIONS, TOKENS, D)
    entries = jnp.clip(jax.random.normal(jax.random.fold_in(key, 23), full_shape, jnp.float32), -6.0, 6.0)
    return entries.astype(jnp.bfloat16)


def projection_pair(key):
    full_shape = (SECTIONS, D, INNER)
    leading = jnp.clip(jax.random.normal(jax.random.fold_in(key, 31), full_shape, jnp.float32), -6.0, 6.0) / math.sqrt(D)
    other = jnp.clip(jax.random.normal(jax.random.fold_in(key, 32), full_shape, jnp.float32), -6.0, 6.0) / math.sqrt(D)
    second = other
    return (leading, second)


def draw_w_query(key, part):
    return projection_pair(key)[0].astype(jnp.float32)


def draw_w_key(key, part):
    return projection_pair(key)[1].astype(jnp.float32)


def touch_ends(array, stream_key, smallest, largest):
    longest = array.shape.index(max(array.shape))
    spots = []
    for shift in (0, 1):
        where = [jax.random.randint(jax.random.fold_in(stream_key, axis), (), 0, length) for axis, length in enumerate(array.shape)]
        where[longest] = (where[longest] + shift) % array.shape[longest]
        spots.append(tuple(where))
    return array.at[spots[0]].set(smallest).at[spots[1]].set(largest)


def block_levels(own_key, dims, split, smallest, top_value):
    gain, own = 1.0, jax.random.fold_in(own_key, 6)
    for axis_at, shards_of in split:
        steps = jnp.exp(jax.random.uniform(jax.random.fold_in(own, axis_at), (shards_of,), jnp.float32, smallest / len(split), top_value / len(split)))
        gain = gain * jnp.repeat(steps, dims[axis_at] // shards_of).reshape([-1 if axis == axis_at else 1 for axis in range(len(dims))])
    return gain


def scatter_about(key, shape, deviation, limit, pieces=(), dtype=jnp.bfloat16):
    factor_of = block_levels(key, shape, pieces, -0.22, 0.18) if pieces else 1.0
    drawn = jax.random.normal(key, shape, jnp.float32) * deviation * factor_of
    return jnp.minimum(jnp.maximum(drawn, -limit), limit).astype(dtype)


def setup_inputs(seed: int = 0) -> dict:
    arg_keys = jax.random.split(jax.random.key(seed), 12)
    failed_section = touch_ends(jax.random.randint(arg_keys[0], (REPLICAS,), 0, 1000), jax.random.fold_in(arg_keys[0], 1), 0, 999).astype(jnp.int32)
    token_ids = draw_token_ids(jax.random.fold_in(arg_keys[11], 71), 0)
    section_outputs = draw_section_outputs(jax.random.fold_in(arg_keys[11], 71), 0)
    w_query = draw_w_query(jax.random.fold_in(arg_keys[11], 71), 0)
    w_key = draw_w_key(jax.random.fold_in(arg_keys[11], 71), 0)
    w_value = scatter_about(arg_keys[5], (SECTIONS, D, INNER), D ** -0.5, 0.125, ((0, 4), (1, 8), (2, 4)), jnp.float32)
    w_out = scatter_about(arg_keys[6], (SECTIONS, D, INNER), (INNER // 16) ** -0.5, 0.75, ((0, 4), (1, 8), (2, 4)), jnp.float32)
    m_value = scatter_about(arg_keys[7], (SECTIONS, D, INNER), 0.5, 3.0, ((0, 4), (1, 8), (2, 4)), jnp.float32)
    v_value = jnp.clip(jnp.exp(math.log(1.0) - 6.9077552 * jax.random.uniform(arg_keys[8], (SECTIONS, D, INNER), jnp.float32) ** block_levels(arg_keys[8], (SECTIONS, D, INNER), ((0, 4), (1, 8), (2, 4)), -0.2, 0.2)), 0.001, 1.0)
    m_out = scatter_about(arg_keys[9], (SECTIONS, D, INNER), 0.5, 3.0, ((0, 4), (1, 8), (2, 4)), jnp.float32)
    v_out = jnp.clip(jnp.exp(math.log(1.0) - 6.9077552 * jax.random.uniform(arg_keys[10], (SECTIONS, D, INNER), jnp.float32) ** block_levels(arg_keys[10], (SECTIONS, D, INNER), ((0, 4), (1, 8), (2, 4)), -0.2, 0.2)), 0.001, 1.0)
    return {"failed_section": failed_section, "token_ids": token_ids, "section_outputs": section_outputs, "w_query": w_query, "w_key": w_key, "w_value": w_value, "w_out": w_out, "m_value": m_value, "v_value": v_value, "m_out": m_out, "v_out": v_out}


end_token = 100001
mask_fill = -1e+30

def document_ids(token_row):
    doc_ends = (token_row == end_token).astype(jnp.int32)
    return jnp.cumsum(doc_ends) - doc_ends

def attend_head(query_head, key_head, value_head, allowed):
    scores = jnp.dot(query_head, key_head.T, preferred_element_type=jnp.float32) * (1.0 / math.sqrt(HD))
    scores = jnp.where(allowed, scores, mask_fill)
    highest = lax.optimization_barrier(jnp.max(scores, axis=1, keepdims=True))
    weights = jnp.exp(scores - highest)
    probs = (weights / lax.optimization_barrier(jnp.sum(weights, axis=1, keepdims=True))).astype(jnp.bfloat16)
    return jnp.dot(probs, value_head, preferred_element_type=jnp.float32).astype(jnp.bfloat16)

def recompute(incoming, token_row, query_master, key_master, value_master, out_master):
    queries = jnp.dot(incoming, query_master.astype(jnp.bfloat16), preferred_element_type=jnp.float32).astype(jnp.bfloat16)
    key_vals = jnp.dot(incoming, key_master.astype(jnp.bfloat16), preferred_element_type=jnp.float32).astype(jnp.bfloat16)
    value_vals = jnp.dot(incoming, value_master.astype(jnp.bfloat16), preferred_element_type=jnp.float32).astype(jnp.bfloat16)
    query_heads = queries.reshape(TOKENS, HEADS, HD).transpose(1, 0, 2)
    key_heads = key_vals.reshape(TOKENS, HEADS, HD).transpose(1, 0, 2)
    value_heads = value_vals.reshape(TOKENS, HEADS, HD).transpose(1, 0, 2)
    document = document_ids(token_row)
    positions = jnp.arange(TOKENS)
    allowed = (positions[None, :] <= positions[:, None]) & (document[None, :] == document[:, None])
    context = lax.map(lambda trio: attend_head(trio[0], trio[1], trio[2], allowed), (query_heads, key_heads, value_heads))
    context = context.transpose(1, 0, 2).reshape(TOKENS, INNER)
    return jnp.dot(context, out_master.astype(jnp.bfloat16).T, preferred_element_type=jnp.float32).astype(jnp.bfloat16)

def reference(failed_section, token_ids, section_outputs, w_query, w_key, w_value, w_out, m_value, v_value, m_out, v_out):
    sources = (w_query, w_key, w_value, w_out, m_value, v_value, m_out, v_out)
    results = [jnp.zeros((REPLICAS, SECTIONS, D, INNER), jnp.float32) for item in sources]
    update_all = jnp.zeros((REPLICAS, SECTIONS, TOKENS, D), jnp.bfloat16)
    for replica in range(REPLICAS):
        section_failed = jnp.remainder(failed_section[replica], SECTIONS).astype(jnp.int32)
        before = jnp.remainder(section_failed + SECTIONS - 1, SECTIONS).astype(jnp.int32)
        incoming = section_outputs[replica, before]
        blocks = [source[section_failed] for source in sources]
        update = recompute(incoming, token_ids[replica], blocks[0], blocks[1], blocks[2], blocks[3])
        results = [result.at[replica, section_failed].set(block) for result, block in zip(results, blocks)]
        update_all = update_all.at[replica, section_failed].set(update)
    return (results[0], results[1], results[2], results[3], results[4], results[5], results[6], results[7], update_all)
```

```python
import math

import jax
import jax.numpy as jnp
from jax import lax
from jax.experimental import pallas as pl
from jax.experimental.pallas import tpu as pltpu
from jax.sharding import PartitionSpec as P

MESH = pl.DeviceIdType.MESH
HD = 128
END_TOKEN = 100001
FILL = -1e30
SCALE = 1.0 / math.sqrt(HD)

ROWS = 2048
CHUNK = 256
STEPS = ROWS // CHUNK
SHARD = 256
FEATS = 512
HALF = SHARD // 2

GROUPS = ((0, 3), (3, 1), (4, 1), (5, 1), (6, 1), (7, 1))
LOOP = 12


def produced(i):
    return jnp.clip(jnp.minimum(2 * (i - 4), i - 1), 0, STEPS)


def gather_attend(
    tok, x, wq, wk, wv, wo, mv, vv, mo, vo,
    full, ctx_full, wo_rows,
    own, xs, wb, qb, kb, vb, cb, ends, bounce,
    w_send, w_recv, x_send, x_recv, c_send, c_recv, o_send, o_recv, local_sem,
):
    r = lax.axis_index("dp")
    s = lax.axis_index("section")
    t = lax.axis_index("tensor")
    zh, xi = r // 4, r % 4
    right = zh * 4 + (xi + 1) % 4
    left = zh * 4 + (xi + 3) % 4
    twin = (r + 4) % 8
    down = (s + 1) % 4
    up = (s + 3) % 4
    core = (t // 2) * 2 + (t + 1) % 2
    pair = (t + 2) % 4
    cross = (core + 2) % 4

    for index, ref in enumerate((wq, wk, wv, wo, mv, vv, mo, vo)):
        own[index] = ref[...].astype(jnp.bfloat16)

    barrier = pltpu.get_barrier_semaphore()
    peers = (
        {"dp": right}, {"dp": left}, {"dp": twin}, {"section": down}, {"section": up},
        {"tensor": core}, {"tensor": pair}, {"tensor": cross},
    )
    for peer in peers:
        pl.semaphore_signal(barrier, inc=1, device_id=peer, device_id_type=MESH)
    pl.semaphore_wait(barrier, len(peers))

    def remote(src, dst, send, recv, to):
        return pltpu.make_async_remote_copy(
            src_ref=src, dst_ref=dst, send_sem=send, recv_sem=recv, device_id=to, device_id_type=MESH
        )

    def place(g, block, first=0, count=SHARD):
        start, n = GROUPS[g]
        return full.at[pl.ds(start, n), pl.ds(pl.multiple_of(block * SHARD + first, HALF), count), :]

    def w_copy(g, kind):
        start, n = GROUPS[g]
        mine = own.at[pl.ds(start, n)]
        sems = w_send.at[g, kind], w_recv.at[g, kind]
        if kind == 0:
            return remote(mine, place(g, r), *sems, {"dp": twin})
        if kind == 1:
            return remote(mine, place(g, r), *sems, {"dp": right})
        if kind == 2:
            return remote(mine, place(g, r), *sems, {"dp": left})
        if kind == 3:
            return remote(place(g, twin), place(g, twin), *sems, {"dp": right})
        if kind == 4:
            return remote(place(g, twin), place(g, twin), *sems, {"dp": left})
        source = (left, right, (left + 4) % 8, (right + 4) % 8)[kind - 5]
        to = right if kind in (5, 7) else left
        half = place(g, source, 0 if kind in (5, 7) else HALF, HALF)
        return remote(half, half, *sems, {"dp": to})

    def w_own(g):
        w_copy(g, 0).start()
        w_copy(g, 1).start()
        w_copy(g, 2).start()

    def w_twin(g):
        w_copy(g, 0).wait_recv()
        w_copy(g, 3).start()
        w_copy(g, 4).start()

    def w_on(g):
        for kind in (1, 2):
            w_copy(g, kind).wait_recv()
            w_copy(g, kind + 4).start()

    def w_twin_on(g):
        for kind in (3, 4):
            w_copy(g, kind).wait_recv()
            w_copy(g, kind + 4).start()

    def w_whole(g):
        for kind in (5, 6, 7, 8):
            w_copy(g, kind).wait_recv()

    def rows(c):
        return pl.ds(pl.multiple_of(c * CHUNK, CHUNK), CHUNK)

    def x_copy(c, kind):
        sems = x_send.at[kind, c], x_recv.at[kind, c]
        if kind == 0:
            return remote(x.at[rows(c), :], xs.at[t, rows(c), :], *sems, {"section": down})
        slot = pair if kind == 3 else t
        part = xs.at[slot, rows(c), :]
        return remote(part, part, *sems, {"tensor": pair if kind == 1 else core})

    def c_copy(c, kind):
        sems = c_send.at[kind, c], c_recv.at[kind, c]
        if kind == 2:
            part = ctx_full.at[pair, rows(c), :]
            return remote(part, part, *sems, {"tensor": core})
        return remote(cb.at[rows(c), :], ctx_full.at[t, rows(c), :], *sems, {"tensor": pair if kind == 0 else core})

    def o_copy(kind):
        to = (pair, core, cross)[kind]
        src = full.at[3, pl.ds(pl.multiple_of(to * FEATS, FEATS), FEATS), :]
        return remote(src, wo_rows.at[t], o_send.at[kind], o_recv.at[kind], {"tensor": to})

    w_own(0)
    lax.fori_loop(0, STEPS, lambda c, _: (x_copy(c, 0).start(), 0)[1], 0)
    keep = [
        pltpu.make_async_copy(own.at[pl.ds(n0, n)], place(g, r), local_sem.at[g])
        for g, (n0, n) in enumerate(GROUPS)
    ]
    for copy in keep:
        copy.start()
    where = lax.broadcasted_iota(jnp.int32, (1, ROWS), 1).astype(jnp.float32)
    ends[...] = jnp.where(tok[...] == END_TOKEN, where + 1.0, 0.0)

    def attend(c, _):
        for kind in (2, 3):
            x_copy(c, kind).wait_recv()
        for a, dst in enumerate((qb, kb, vb)):
            total = jnp.zeros((CHUNK, SHARD), jnp.float32)
            for part in range(4):
                total += jnp.dot(
                    xs[part, rows(c), :], wb[a, part * FEATS : (part + 1) * FEATS, :],
                    preferred_element_type=jnp.float32,
                )
            if a == 0:
                dst[...] = total.astype(jnp.bfloat16)
            else:
                dst[rows(c), :] = total.astype(jnp.bfloat16)
        row = (c * CHUNK + lax.broadcasted_iota(jnp.int32, (CHUNK, 1), 0)).astype(jnp.float32)
        first = jnp.max(jnp.where(where < row, ends[...], 0.0), axis=1, keepdims=True)

        def step(j, carry):
            col = (j * CHUNK + lax.broadcasted_iota(jnp.int32, (1, CHUNK), 1)).astype(jnp.float32)
            allowed = (col <= row) & (col >= first)
            new = []
            for h in range(2):
                highest, total, acc = carry[h]
                lanes = slice(h * HD, (h + 1) * HD)
                scores = lax.dot_general(
                    qb[:, lanes], kb[rows(j), lanes], (((1,), (1,)), ((), ())),
                    preferred_element_type=jnp.float32,
                ) * SCALE
                scores = jnp.where(allowed, scores, FILL)
                top = jnp.maximum(highest, jnp.max(scores, axis=1, keepdims=True))
                weights = jnp.exp(scores - top)
                shrink = jnp.exp(highest - top)
                total = total * shrink + jnp.sum(weights, axis=1, keepdims=True)
                acc = acc * shrink + jnp.dot(
                    weights.astype(jnp.bfloat16), vb[rows(j), lanes], preferred_element_type=jnp.float32
                )
                new.append((top, total, acc))
            return tuple(new)

        begin = (
            jnp.full((CHUNK, 1), FILL, jnp.float32),
            jnp.zeros((CHUNK, 1), jnp.float32),
            jnp.zeros((CHUNK, HD), jnp.float32),
        )
        done = lax.fori_loop(0, c + 1, step, (begin, begin))
        for h in range(2):
            _, total, acc = done[h]
            cb[rows(c), h * HD : (h + 1) * HD] = (acc / total).astype(jnp.bfloat16)
        return 0

    def send_context(c, _):
        c_copy(c, 0).start()
        c_copy(c, 1).start()
        pltpu.make_async_copy(cb.at[rows(c), :], ctx_full.at[t, rows(c), :], c_send.at[3, c]).start()
        return 0

    events = {step: [] for step in range(LOOP)}
    events[1] += [(w_twin, 0), (w_on, 0)]
    events[3] += [(w_twin_on, 0)]
    events[5] += [(w_whole, 0)]
    for g in range(1, 6):
        events[g] += [(w_own, g)]
        events[g + 2] += [(w_on, g)]
        events[g + 3] += [(w_twin, g)]
        events[g + 6] += [(w_twin_on, g)]

    def loop(i, _):
        @pl.when(i < STEPS)
        def _():
            x_copy(i, 0).wait_recv()
            x_copy(i, 1).start()
            x_copy(i, 2).start()

        for at, todo in events.items():
            if todo:
                @pl.when(i == at)
                def _(todo=todo, at=at):
                    for act, g in todo:
                        act(g)
                    if at == 5:
                        for copy in keep:
                            copy.wait()
                        load = pltpu.make_async_copy(full.at[pl.ds(0, 3)], wb, local_sem.at[6])
                        load.start()
                        load.wait()

        @pl.when((i >= 2) & (i < STEPS + 2))
        def _():
            x_copy(i - 2, 1).wait_recv()
            x_copy(i - 2, 3).start()

        lax.fori_loop(produced(i - 2), produced(i - 1), send_context, 0)
        lax.fori_loop(produced(i - 1), produced(i), attend, 0)
        return 0

    lax.fori_loop(0, LOOP, loop, 0)

    w_whole(1)
    for kind in range(3):
        o_copy(kind).start()
    mine = pl.ds(pl.multiple_of(t * FEATS, FEATS), FEATS)
    load = pltpu.make_async_copy(full.at[3, mine, :], bounce, local_sem.at[6])
    load.start()
    load.wait()
    store = pltpu.make_async_copy(bounce, wo_rows.at[t], local_sem.at[6])
    store.start()

    def forward_context(c, _):
        c_copy(c, 0).wait_recv()
        c_copy(c, 2).start()
        return 0

    lax.fori_loop(0, STEPS, forward_context, 0)
    for g in range(2, 6):
        w_whole(g)
    for kind in range(3):
        o_copy(kind).wait()
    store.wait()

    def finish(c, _):
        for kind in range(4):
            x_copy(c, kind).wait_send()
        c_copy(c, 0).wait_send()
        c_copy(c, 1).wait()
        c_copy(c, 2).wait()
        pltpu.make_async_copy(cb.at[rows(c), :], ctx_full.at[t, rows(c), :], c_send.at[3, c]).wait()
        return 0

    lax.fori_loop(0, STEPS, finish, 0)
    for g in range(6):
        for kind in range(9):
            w_copy(g, kind).wait_send()


def place_blocks(failed, full, ctx, wo_rows, *outs):
    replacing = lax.rem(failed[0], 4) == lax.axis_index("section")
    for a in range(8):
        outs[a][0, 0] = jnp.where(replacing, full[a].astype(jnp.float32), 0.0)
    total = jnp.zeros((CHUNK, FEATS), jnp.float32)
    for part in range(4):
        total += lax.dot_general(
            ctx[part], wo_rows[part], (((1,), (1,)), ((), ())), preferred_element_type=jnp.float32
        )
    outs[8][0, 0] = jnp.where(replacing, total, 0.0).astype(jnp.bfloat16)


def shards(failed_section, token_ids, section_outputs, *weights):
    bf16 = jnp.bfloat16
    vmem = pl.BlockSpec(memory_space=pltpu.VMEM)
    hbm = pl.BlockSpec(memory_space=pl.ANY)
    dma = pltpu.SemaphoreType.DMA
    full, ctx, wo_rows = pl.pallas_call(
        gather_attend,
        out_shape=(
            jax.ShapeDtypeStruct((8, ROWS, SHARD), bf16),
            jax.ShapeDtypeStruct((4, ROWS, SHARD), bf16),
            jax.ShapeDtypeStruct((4, FEATS, SHARD), bf16),
        ),
        in_specs=[vmem, hbm] + [vmem] * 8,
        out_specs=(hbm, hbm, hbm),
        scratch_shapes=[
            pltpu.VMEM((8, SHARD, SHARD), bf16),
            pltpu.VMEM((4, ROWS, FEATS), bf16),
            pltpu.VMEM((3, ROWS, SHARD), bf16),
            pltpu.VMEM((CHUNK, SHARD), bf16),
            pltpu.VMEM((ROWS, SHARD), bf16),
            pltpu.VMEM((ROWS, SHARD), bf16),
            pltpu.VMEM((ROWS, SHARD), bf16),
            pltpu.VMEM((1, ROWS), jnp.float32),
            pltpu.VMEM((FEATS, SHARD), bf16),
            dma((6, 9)),
            dma((6, 9)),
            dma((4, STEPS)),
            dma((4, STEPS)),
            dma((4, STEPS)),
            dma((3, STEPS)),
            dma((3,)),
            dma((3,)),
            dma((7,)),
        ],
        compiler_params=pltpu.CompilerParams(
            collective_id=0, has_side_effects=True, vmem_limit_bytes=60 * 2**20
        ),
    )(
        token_ids,
        section_outputs.reshape(ROWS, FEATS),
        *(w.reshape(SHARD, SHARD) for w in weights),
    )
    wide = jax.ShapeDtypeStruct((1, 1, ROWS, SHARD), jnp.float32)
    return pl.pallas_call(
        place_blocks,
        grid=(STEPS,),
        out_shape=(wide,) * 8 + (jax.ShapeDtypeStruct((1, 1, ROWS, FEATS), bf16),),
        in_specs=[
            pl.BlockSpec(memory_space=pltpu.SMEM),
            pl.BlockSpec((8, CHUNK, SHARD), lambda i: (0, i, 0)),
            pl.BlockSpec((4, CHUNK, SHARD), lambda i: (0, i, 0)),
            pl.BlockSpec((4, FEATS, SHARD), lambda i: (0, 0, 0)),
        ],
        out_specs=[pl.BlockSpec((1, 1, CHUNK, SHARD), lambda i: (0, 0, i, 0))] * 8
        + [pl.BlockSpec((1, 1, CHUNK, FEATS), lambda i: (0, 0, i, 0))],
        compiler_params=pltpu.CompilerParams(vmem_limit_bytes=60 * 2**20),
    )(failed_section, full, ctx, wo_rows)


def solution(mesh):
    stack = P("section", "dp", "tensor")
    block = P("dp", "section", None, "tensor")
    return jax.shard_map(
        shards,
        mesh=mesh,
        in_specs=(P("dp"), P("dp", None), block) + (stack,) * 8,
        out_specs=(block,) * 9,
        check_vma=False,
    )
```

```python
import math

import jax
import jax.numpy as jnp
from jax import lax
from jax.experimental import pallas as pl
from jax.experimental.pallas import tpu as pltpu
from jax.sharding import PartitionSpec as P

MESH = pl.DeviceIdType.MESH
HD = 128
END_TOKEN = 100001
FILL = -1e30
SCALE = 1.0 / math.sqrt(HD)

ROWS = 2048
CHUNK = 256
STEPS = ROWS // CHUNK
SHARD = 256
FEATS = 512
HALF = SHARD // 2

GROUPS = ((0, 3), (3, 1), (4, 1), (5, 1), (6, 1), (7, 1))
LAST = 9


def produced(i):
    return jnp.clip(jnp.maximum(3 * i - 10, 0) // 2, 0, STEPS)


def gather_attend(
    failed, tok, x, wq, wk, wv, wo, mv, vv, mo, vo,
    full, ctx_full, wo_rows,
    xs, early, swap, qb, kb, vb, ends,
    w_send, w_recv, x_send, x_recv, c_send, c_recv, o_send, o_recv, local_sem,
):
    r = lax.axis_index("dp")
    s = lax.axis_index("section")
    t = lax.axis_index("tensor")
    zh, xi = r // 4, r % 4
    right = zh * 4 + (xi + 1) % 4
    left = zh * 4 + (xi + 3) % 4
    twin = (r + 4) % 8
    down = (s + 1) % 4
    up = (s + 3) % 4
    core = (t // 2) * 2 + (t + 1) % 2
    pair = (t + 2) % 4
    cross = (core + 2) % 4
    source = lax.rem(failed[0] + 3, 4) == s

    def rows(c):
        return pl.ds(pl.multiple_of(c * CHUNK, CHUNK), CHUNK)

    loads = [
        pltpu.make_async_copy(x.at[rows(2 * m + 1), :], early.at[m], local_sem.at[m])
        for m in range(STEPS // 2)
    ]
    for load in loads:
        load.start()
    for index, ref in enumerate((wq, wk, wv, wo, mv, vv, mo, vo)):
        full[index, pl.ds(pl.multiple_of(r * SHARD, SHARD), SHARD), :] = ref[...].astype(jnp.bfloat16)

    barrier = pltpu.get_barrier_semaphore()
    peers = (
        {"dp": right}, {"dp": left}, {"dp": twin}, {"section": down}, {"section": up},
        {"tensor": core}, {"tensor": pair}, {"tensor": cross},
    )
    for peer in peers:
        pl.semaphore_signal(barrier, inc=1, device_id=peer, device_id_type=MESH)
    pl.semaphore_wait(barrier, len(peers))

    def remote(src, dst, send, recv, to):
        return pltpu.make_async_remote_copy(
            src_ref=src, dst_ref=dst, send_sem=send, recv_sem=recv, device_id=to, device_id_type=MESH
        )

    def w_copy(g, kind):
        start, n = GROUPS[g]
        block = (r, r, r, twin, twin, left, right, (left + 4) % 8, (right + 4) % 8)[kind]
        to = (twin, right, left, right, left, right, left, right, left)[kind]
        first = HALF if kind in (6, 8) else 0
        count = HALF if kind >= 5 else SHARD
        part = full.at[pl.ds(start, n), pl.ds(pl.multiple_of(block * SHARD + first, HALF), count), :]
        return remote(part, part, w_send.at[g, kind], w_recv.at[g, kind], {"dp": to})

    def w_own(g):
        for kind in (0, 1, 2):
            w_copy(g, kind).start()

    def w_twin(g):
        w_copy(g, 0).wait_recv()
        w_copy(g, 3).start()
        w_copy(g, 4).start()

    def w_on(g):
        for kind in (1, 2):
            w_copy(g, kind).wait_recv()
            w_copy(g, kind + 4).start()

    def w_twin_on(g):
        for kind in (3, 4):
            w_copy(g, kind).wait_recv()
            w_copy(g, kind + 4).start()

    def w_whole(g):
        for kind in (5, 6, 7, 8):
            w_copy(g, kind).wait_recv()

    def x_copy(c, kind):
        sems = x_send.at[kind, c], x_recv.at[kind, c]
        if kind == 0:
            return remote(x.at[rows(c), :], xs.at[t, rows(c), :], *sems, {"section": down})
        if kind == 1:
            return remote(swap.at[c // 2], xs.at[t, rows(c), :], *sems, {"tensor": pair})
        if kind == 4:
            return remote(xs.at[pair, rows(c - 1), :], xs.at[pair, rows(c), :], *sems, {"section": down})
        part = xs.at[t if kind == 2 else pair, rows(c), :]
        return remote(part, part, *sems, {"tensor": core})

    def x_own(c):
        x_copy(c, 0).start()

    def x_wait(c):
        x_copy(c, 0).wait_recv()

    def x_share(c):
        x_copy(c, 2).start()

    def x_swap(c):
        loads[c // 2].wait()
        swap[c // 2] = jnp.where(source, early[c // 2], xs[t, rows(c), :])

    def x_swap_send(c):
        x_copy(c, 1).start()

    def x_swapped(c):
        x_copy(c, 1).wait_recv()
        x_copy(c + 1, 4).start()
        x_copy(c, 3).start()

    def x_other(c):
        x_copy(c, 4).wait_recv()
        x_copy(c, 3).start()

    def c_copy(c, kind):
        sems = c_send.at[kind, c], c_recv.at[kind, c]
        part = ctx_full.at[pair if kind == 2 else t, rows(c), :]
        return remote(part, part, *sems, {"tensor": pair if kind == 0 else core})

    def o_copy(kind):
        to = (pair, core, cross)[kind]
        src = full.at[3, pl.ds(pl.multiple_of(to * FEATS, FEATS), FEATS), :]
        return remote(src, wo_rows.at[t], o_send.at[kind], o_recv.at[kind], {"tensor": to})

    def o_all(_):
        w_whole(1)
        for kind in range(3):
            o_copy(kind).start()
        wo_rows[t] = full[3, pl.ds(pl.multiple_of(t * FEATS, FEATS), FEATS), :]

    where = lax.broadcasted_iota(jnp.int32, (1, ROWS), 1).astype(jnp.float32)
    ends[...] = jnp.where(tok[...] == END_TOKEN, where + 1.0, 0.0)

    def attend(c, _):
        for kind in (2, 3):
            x_copy(c, kind).wait_recv()
        for a, dst in enumerate((qb, kb, vb)):
            total = jnp.zeros((CHUNK, SHARD), jnp.float32)
            for part in range(4):
                total += jnp.dot(
                    xs[part, rows(c), :], full[a, part * FEATS : (part + 1) * FEATS, :],
                    preferred_element_type=jnp.float32,
                )
            if a == 0:
                dst[...] = total.astype(jnp.bfloat16)
            else:
                dst[rows(c), :] = total.astype(jnp.bfloat16)
        row = (c * CHUNK + lax.broadcasted_iota(jnp.int32, (CHUNK, 1), 0)).astype(jnp.float32)
        first = jnp.max(jnp.where(where < row, ends[...], 0.0), axis=1, keepdims=True)

        def step(j, carry):
            col = (j * CHUNK + lax.broadcasted_iota(jnp.int32, (1, CHUNK), 1)).astype(jnp.float32)
            allowed = (col <= row) & (col >= first)
            new = []
            for h in range(2):
                highest, total, acc = carry[h]
                lanes = slice(h * HD, (h + 1) * HD)
                scores = lax.dot_general(
                    qb[:, lanes], kb[rows(j), lanes], (((1,), (1,)), ((), ())),
                    preferred_element_type=jnp.float32,
                ) * SCALE
                scores = jnp.where(allowed, scores, FILL)
                top = jnp.maximum(highest, jnp.max(scores, axis=1, keepdims=True))
                weights = jnp.exp(scores - top)
                shrink = jnp.exp(highest - top)
                total = total * shrink + jnp.sum(weights, axis=1, keepdims=True)
                acc = acc * shrink + jnp.dot(
                    weights.astype(jnp.bfloat16), vb[rows(j), lanes], preferred_element_type=jnp.float32
                )
                new.append((top, total, acc))
            return tuple(new)

        begin = (
            jnp.full((CHUNK, 1), FILL, jnp.float32),
            jnp.zeros((CHUNK, 1), jnp.float32),
            jnp.zeros((CHUNK, HD), jnp.float32),
        )
        done = lax.fori_loop(0, c + 1, step, (begin, begin))
        for h in range(2):
            _, total, acc = done[h]
            ctx_full[t, rows(c), h * HD : (h + 1) * HD] = (acc / total).astype(jnp.bfloat16)
        return 0

    def send_context(c, _):
        c_copy(c, 0).start()
        c_copy(c, 1).start()
        return 0

    before = {
        1: [(w_twin, 0), (w_on, 0), (w_own, 3), (x_swapped, 0), (x_own, 3), (x_own, 4)],
        2: [],
        3: [(w_twin_on, 0), (w_twin, 1), (w_on, 2), (x_swapped, 2), (x_own, 5), (x_own, 6), (w_own, 5)],
        4: [],
        5: [(w_twin_on, 1), (w_twin, 4), (w_on, 4), (x_swapped, 4), (x_own, 7)],
        6: [(x_other, 3)],
        7: [(x_swapped, 6), (w_twin_on, 3), (o_all, 0)],
        8: [(x_other, 5)],
        9: [(w_twin_on, 4), (w_twin_on, 5), (x_other, 7)],
    }
    for c in range(STEPS):
        if c % 2 == 0:
            before[c] = [(x_wait, c), (x_swap, c), (x_share, c)] + before.get(c, [])
    before[0] += [(x_swap_send, 0), (w_own, 1), (w_own, 2)]
    before[2] += [(x_swap_send, 2), (w_on, 1), (w_own, 4)]
    before[4] += [(x_swap_send, 4), (x_other, 1), (w_on, 3), (w_twin, 2), (w_twin, 3), (w_whole, 0)]
    before[6] += [(x_swap_send, 6), (w_on, 5), (w_twin_on, 2), (w_twin, 5)]
    after = {c: [(x_wait, c), (x_share, c)] for c in range(1, STEPS, 2)}

    def run(i, table):
        for at, todo in table.items():
            @pl.when(i == at)
            def _(todo=todo):
                for act, what in todo:
                    act(what)

    w_own(0)
    for c in range(3):
        x_own(c)

    def loop(i, _):
        run(i, before)
        lax.fori_loop(produced(i - 2), produced(i - 1), send_context, 0)
        lax.fori_loop(produced(i - 1), produced(i), attend, 0)
        run(i, after)
        return 0

    lax.fori_loop(0, LAST + 1, loop, 0)

    def forward_context(c, _):
        c_copy(c, 0).wait_recv()
        c_copy(c, 2).start()
        return 0

    w_whole(2)
    lax.fori_loop(produced(LAST - 1), STEPS, send_context, 0)
    lax.fori_loop(0, STEPS, forward_context, 0)
    for g in range(3, 6):
        w_whole(g)
    for kind in range(3):
        o_copy(kind).wait()

    def finish(c, _):
        for kind in (0, 2, 3):
            x_copy(c, kind).wait_send()
        c_copy(c, 0).wait_send()
        c_copy(c, 1).wait()
        c_copy(c, 2).wait()
        return 0

    lax.fori_loop(0, STEPS, finish, 0)
    for c in range(0, STEPS, 2):
        x_copy(c, 1).wait_send()
        x_copy(c + 1, 4).wait_send()
    for g in range(6):
        for kind in range(9):
            w_copy(g, kind).wait_send()


def place_blocks(failed, full, ctx, wo_rows, *outs):
    replacing = lax.rem(failed[0], 4) == lax.axis_index("section")
    here = pl.ds(pl.multiple_of(pl.program_id(0) * CHUNK, CHUNK), CHUNK)
    for a in range(8):
        outs[a][0, 0] = jnp.where(replacing, full[a, here, :].astype(jnp.float32), 0.0)
    total = jnp.zeros((CHUNK, FEATS), jnp.float32)
    for part in range(4):
        total += lax.dot_general(
            ctx[part, here, :], wo_rows[part], (((1,), (1,)), ((), ())), preferred_element_type=jnp.float32
        )
    outs[8][0, 0] = jnp.where(replacing, total, 0.0).astype(jnp.bfloat16)


def shards(failed_section, token_ids, section_outputs, *weights):
    bf16 = jnp.bfloat16
    vmem = pl.BlockSpec(memory_space=pltpu.VMEM)
    hbm = pl.BlockSpec(memory_space=pl.ANY)
    dma = pltpu.SemaphoreType.DMA
    full, ctx, wo_rows = pl.pallas_call(
        gather_attend,
        out_shape=(
            pltpu.VMEM((8, ROWS, SHARD), bf16),
            pltpu.VMEM((4, ROWS, SHARD), bf16),
            pltpu.VMEM((4, FEATS, SHARD), bf16),
        ),
        in_specs=[pl.BlockSpec(memory_space=pltpu.SMEM), vmem, hbm] + [vmem] * 8,
        out_specs=(vmem, vmem, vmem),
        scratch_shapes=[
            pltpu.VMEM((4, ROWS, FEATS), bf16),
            pltpu.VMEM((STEPS // 2, CHUNK, FEATS), bf16),
            pltpu.VMEM((STEPS // 2, CHUNK, FEATS), bf16),
            pltpu.VMEM((CHUNK, SHARD), bf16),
            pltpu.VMEM((ROWS, SHARD), bf16),
            pltpu.VMEM((ROWS, SHARD), bf16),
            pltpu.VMEM((1, ROWS), jnp.float32),
            dma((6, 9)),
            dma((6, 9)),
            dma((5, STEPS)),
            dma((5, STEPS)),
            dma((3, STEPS)),
            dma((3, STEPS)),
            dma((3,)),
            dma((3,)),
            dma((STEPS // 2,)),
        ],
        compiler_params=pltpu.CompilerParams(
            collective_id=0, has_side_effects=True, vmem_limit_bytes=44 * 2**20
        ),
    )(
        failed_section,
        token_ids,
        section_outputs.reshape(ROWS, FEATS),
        *(w.reshape(SHARD, SHARD) for w in weights),
    )
    wide = jax.ShapeDtypeStruct((1, 1, ROWS, SHARD), jnp.float32)
    return pl.pallas_call(
        place_blocks,
        grid=(STEPS,),
        out_shape=(wide,) * 8 + (jax.ShapeDtypeStruct((1, 1, ROWS, FEATS), bf16),),
        in_specs=[
            pl.BlockSpec(memory_space=pltpu.SMEM),
            vmem,
            vmem,
            vmem,
        ],
        out_specs=[pl.BlockSpec((1, 1, CHUNK, SHARD), lambda i: (0, 0, i, 0))] * 8
        + [pl.BlockSpec((1, 1, CHUNK, FEATS), lambda i: (0, 0, i, 0))],
        compiler_params=pltpu.CompilerParams(vmem_limit_bytes=24 * 2**20),
    )(failed_section, full, ctx, wo_rows)


def solution(mesh):
    stack = P("section", "dp", "tensor")
    block = P("dp", "section", None, "tensor")
    return jax.shard_map(
        shards,
        mesh=mesh,
        in_specs=(P("dp"), P("dp", None), block) + (stack,) * 8,
        out_specs=(block,) * 9,
        check_vma=False,
    )
```

```python
import math

import jax
import jax.numpy as jnp
from jax import lax
from jax.experimental import pallas as pl
from jax.experimental.pallas import tpu as pltpu
from jax.sharding import PartitionSpec as P

MESH = pl.DeviceIdType.MESH
HD = 128
END_TOKEN = 100001
FILL = -1e30
SCALE = 1.0 / math.sqrt(HD)

ROWS = 2048
CHUNK = 256
STEPS = ROWS // CHUNK
SHARD = 256
FEATS = 512
HALF = SHARD // 2

GROUPS = ((0, 3), (3, 1), (4, 1), (5, 1), (6, 1), (7, 1))
LAST = 9
LATE = (0, 1, 3, 5)
EARLY = (2, 4, 6, 7)
VIA = (0, 2, 4)


def produced(i):
    return jnp.clip(jnp.minimum(2 * (i - 4), i - 1), 0, STEPS)


def gather_attend(
    failed, tok, x, wq, wk, wv, wo, mv, vv, mo, vo,
    full, ctx_full, wo_rows,
    xs, early, swap, back, lent, cswap, olent, oswap, oback, qb, kb, vb, ends,
    w_send, w_recv, x_send, x_recv, c_send, c_recv, o_send, o_recv, local_sem,
):
    r = lax.axis_index("dp")
    s = lax.axis_index("section")
    t = lax.axis_index("tensor")
    zh, xi = r // 4, r % 4
    right = zh * 4 + (xi + 1) % 4
    left = zh * 4 + (xi + 3) % 4
    twin = (r + 4) % 8
    down = (s + 1) % 4
    up = (s + 3) % 4
    core = (t // 2) * 2 + (t + 1) % 2
    pair = (t + 2) % 4
    cross = (core + 2) % 4
    source = lax.rem(failed[0] + 3, 4) == s

    def rows(c):
        return pl.ds(pl.multiple_of(c * CHUNK, CHUNK), CHUNK)

    loads = [
        pltpu.make_async_copy(x.at[rows(c), :], early.at[k], local_sem.at[k])
        for k, c in enumerate(EARLY + LATE[3:])
    ]
    for load in loads:
        load.start()
    for index, ref in enumerate((wq, wk, wv, wo, mv, vv, mo, vo)):
        full[index, pl.ds(pl.multiple_of(r * SHARD, SHARD), SHARD), :] = ref[...].astype(jnp.bfloat16)

    barrier = pltpu.get_barrier_semaphore()
    peers = (
        {"dp": right}, {"dp": left}, {"dp": twin}, {"section": down}, {"section": up},
        {"tensor": core}, {"tensor": pair}, {"tensor": cross},
    )
    for peer in peers:
        pl.semaphore_signal(barrier, inc=1, device_id=peer, device_id_type=MESH)
    pl.semaphore_wait(barrier, len(peers))

    def remote(src, dst, send, recv, to):
        return pltpu.make_async_remote_copy(
            src_ref=src, dst_ref=dst, send_sem=send, recv_sem=recv, device_id=to, device_id_type=MESH
        )

    def w_copy(g, kind):
        start, n = GROUPS[g]
        block = (r, r, r, twin, twin, left, right, (left + 4) % 8, (right + 4) % 8)[kind]
        to = (twin, right, left, right, left, right, left, right, left)[kind]
        first = HALF if kind in (6, 8) else 0
        count = HALF if kind >= 5 else SHARD
        part = full.at[pl.ds(start, n), pl.ds(pl.multiple_of(block * SHARD + first, HALF), count), :]
        return remote(part, part, w_send.at[g, kind], w_recv.at[g, kind], {"dp": to})

    def w_own(g):
        for kind in (0, 1, 2):
            w_copy(g, kind).start()

    def w_twin(g):
        w_copy(g, 0).wait_recv()
        w_copy(g, 3).start()
        w_copy(g, 4).start()

    def w_on(g):
        for kind in (1, 2):
            w_copy(g, kind).wait_recv()
            w_copy(g, kind + 4).start()

    def w_twin_on(g):
        for kind in (3, 4):
            w_copy(g, kind).wait_recv()
            w_copy(g, kind + 4).start()

    def w_whole(g):
        for kind in (5, 6, 7, 8):
            w_copy(g, kind).wait_recv()

    def x_copy(c, kind):
        sems = x_send.at[kind, c], x_recv.at[kind, c]
        if kind == 0:
            return remote(x.at[rows(c), :], xs.at[t, rows(c), :], *sems, {"section": down})
        if kind == 1:
            return remote(swap.at[LATE.index(c)], xs.at[t, rows(c), :], *sems, {"tensor": pair})
        if kind == 4:
            met = xs.at[pair, rows(LATE[EARLY.index(c)]), :]
            return remote(met, xs.at[pair, rows(c), :], *sems, {"section": down})
        part = xs.at[t if kind == 2 else pair, rows(c), :]
        return remote(part, part, *sems, {"tensor": core})

    def b_copy(j):
        third, fourth = xs.at[t, rows(LATE[2]), :], xs.at[t, rows(LATE[3]), :]
        src = (x.at[rows(LATE[2]), :], swap.at[4], back.at[1], third)[j]
        dst = (back.at[0], back.at[1], third, fourth)[j]
        return remote(src, dst, x_send.at[5, j], x_recv.at[5, j], {"section": up})

    def x_own(c):
        x_copy(c, 0).start()

    def x_wait(c):
        x_copy(c, 0).wait_recv()

    def x_share(c):
        x_copy(c, 2).start()

    def x_swap(c):
        k = LATE.index(c)
        loads[k].wait()
        swap[k] = jnp.where(source, early[k], xs[t, rows(c), :])

    def x_swap_send(c):
        x_copy(c, 1).start()

    def x_swapped(c):
        x_copy(c, 1).wait_recv()
        x_copy(EARLY[LATE.index(c)], 4).start()
        x_copy(c, 3).start()

    def x_other(c):
        x_copy(c, 4).wait_recv()
        x_copy(c, 3).start()

    def b_wait(j):
        b_copy(j).wait_recv()

    def b_send(j):
        b_copy(j).start()

    def b_choose(_):
        loads[4].wait()
        swap[4] = jnp.where(source, early[4], back[0])

    def c_copy(c, kind):
        sems = c_send.at[kind, c], c_recv.at[kind, c]
        mine, other = ctx_full.at[t, rows(c), :], ctx_full.at[pair, rows(c), :]
        if kind == 3:
            return remote(mine, lent.at[VIA.index(c)], *sems, {"section": up})
        if kind == 4:
            return remote(ctx_full.at[pair, rows(c + 1), :], other, *sems, {"section": down})
        if kind == 2:
            return remote(other, other, *sems, {"tensor": core})
        if kind == 0 and c - 1 in VIA:
            return remote(cswap.at[VIA.index(c - 1)], mine, *sems, {"tensor": pair})
        return remote(mine, mine, *sems, {"tensor": pair if kind == 0 else core})

    def c_done(c):
        c_copy(c, 1).start()
        if c in VIA:
            c_copy(c, 3).start()
        elif c - 1 not in VIA:
            c_copy(c, 0).start()

    def c_swap(c):
        k = VIA.index(c)
        c_copy(c, 3).wait_recv()
        cswap[k] = jnp.where(source, lent[k], ctx_full[t, rows(c + 1), :])

    def c_swap_send(c):
        c_copy(c + 1, 0).start()

    def c_swapped(c):
        c_copy(c + 1, 0).wait_recv()
        c_copy(c, 4).start()
        c_copy(c + 1, 2).start()

    def c_back(c):
        c_copy(c, 4).wait_recv()
        c_copy(c, 2).start()

    def o_rows(owner):
        return pl.ds(pl.multiple_of(owner * FEATS, FEATS), FEATS)

    def o_copy(kind):
        src, dst, to = (
            (full.at[3, o_rows(core), :], wo_rows.at[t], {"tensor": core}),
            (full.at[3, o_rows(cross), :], olent, {"section": up}),
            (oswap, wo_rows.at[t], {"tensor": pair}),
            (wo_rows.at[pair], oback, {"section": down}),
            (oback, wo_rows.at[pair], {"tensor": core}),
        )[kind]
        return remote(src, dst, o_send.at[kind], o_recv.at[kind], to)

    def o_first(_):
        w_whole(1)
        o_copy(1).start()
        o_copy(0).start()
        wo_rows[t] = full[3, o_rows(t), :]

    def o_swap(_):
        o_copy(1).wait_recv()
        oswap[...] = jnp.where(source, olent[...], full[3, o_rows(pair), :])

    def o_swap_send(_):
        o_copy(2).start()

    def o_swapped(_):
        o_copy(2).wait_recv()
        o_copy(3).start()

    def o_back(_):
        o_copy(3).wait_recv()
        o_copy(4).start()

    where = lax.broadcasted_iota(jnp.int32, (1, ROWS), 1).astype(jnp.float32)
    ends[...] = jnp.where(tok[...] == END_TOKEN, where + 1.0, 0.0)

    def attend(c, _):
        for kind in (2, 3):
            x_copy(c, kind).wait_recv()
        for a, dst in enumerate((qb, kb, vb)):
            total = jnp.zeros((CHUNK, SHARD), jnp.float32)
            for part in range(4):
                total += jnp.dot(
                    xs[part, rows(c), :], full[a, part * FEATS : (part + 1) * FEATS, :],
                    preferred_element_type=jnp.float32,
                )
            if a == 0:
                dst[...] = total.astype(jnp.bfloat16)
            else:
                dst[rows(c), :] = total.astype(jnp.bfloat16)
        row = (c * CHUNK + lax.broadcasted_iota(jnp.int32, (CHUNK, 1), 0)).astype(jnp.float32)
        first = jnp.max(jnp.where(where < row, ends[...], 0.0), axis=1, keepdims=True)

        def step(j, carry):
            col = (j * CHUNK + lax.broadcasted_iota(jnp.int32, (1, CHUNK), 1)).astype(jnp.float32)
            allowed = (col <= row) & (col >= first)
            new = []
            for h in range(2):
                highest, total, acc = carry[h]
                lanes = slice(h * HD, (h + 1) * HD)
                scores = lax.dot_general(
                    qb[:, lanes], kb[rows(j), lanes], (((1,), (1,)), ((), ())),
                    preferred_element_type=jnp.float32,
                ) * SCALE
                scores = jnp.where(allowed, scores, FILL)
                top = jnp.maximum(highest, jnp.max(scores, axis=1, keepdims=True))
                weights = jnp.exp(scores - top)
                shrink = jnp.exp(highest - top)
                total = total * shrink + jnp.sum(weights, axis=1, keepdims=True)
                acc = acc * shrink + jnp.dot(
                    weights.astype(jnp.bfloat16), vb[rows(j), lanes], preferred_element_type=jnp.float32
                )
                new.append((top, total, acc))
            return tuple(new)

        begin = (
            jnp.full((CHUNK, 1), FILL, jnp.float32),
            jnp.zeros((CHUNK, 1), jnp.float32),
            jnp.zeros((CHUNK, HD), jnp.float32),
        )
        done = lax.fori_loop(0, c + 1, step, (begin, begin))
        for h in range(2):
            _, total, acc = done[h]
            ctx_full[t, rows(c), h * HD : (h + 1) * HD] = (acc / total).astype(jnp.bfloat16)
        return 0

    before = {
        0: [
            (x_wait, 0), (x_swap, 0), (x_share, 0), (b_wait, 0), (b_choose, 0), (x_swap_send, 0),
            (w_own, 1), (b_send, 1),
        ],
        1: [
            (w_twin, 0), (w_on, 0), (x_wait, 1), (x_swap, 1), (x_share, 1),
            (b_wait, 1), (b_send, 2), (x_swap_send, 1),
        ],
        2: [(x_swapped, 0), (x_own, 6), (w_twin, 1), (w_on, 1), (x_wait, 2), (x_share, 2)],
        3: [
            (b_wait, 2), (b_send, 3), (x_swap, 3), (x_share, 3), (w_twin_on, 0),
            (x_swap_send, 3), (w_own, 2), (w_own, 3),
        ],
        4: [(x_swapped, 1), (x_own, 7), (x_wait, 4), (x_share, 4), (w_twin_on, 1)],
        5: [
            (b_wait, 3), (x_swap, 5), (x_share, 5), (w_own, 4), (x_swap_send, 5), (w_own, 5), (w_whole, 0),
        ],
        6: [
            (x_swapped, 3), (x_other, 2), (c_done, 0), (c_done, 1), (x_wait, 6), (x_share, 6),
            (w_on, 2), (w_twin, 2),
        ],
        7: [
            (x_swapped, 5), (x_other, 4), (c_swap, 0), (c_done, 2), (c_done, 3), (c_swap_send, 0),
            (o_first, 0), (w_on, 3), (w_twin, 3), (w_on, 4), (w_twin, 4), (x_wait, 7), (x_share, 7),
        ],
        8: [
            (x_other, 6), (c_swap, 2), (o_swap, 0), (c_done, 4), (c_done, 5), (c_swap_send, 2), (o_swap_send, 0),
            (c_swapped, 0), (w_on, 5), (w_twin, 5), (w_twin_on, 2),
        ],
        9: [
            (x_other, 7), (c_swap, 4), (c_done, 6), (c_swap_send, 4), (c_swapped, 2), (o_swapped, 0),
            (w_twin_on, 3), (c_back, 0),
        ],
    }
    tail = [
        (w_twin_on, 4), (c_done, 7), (c_swapped, 4), (w_twin_on, 5), (c_back, 2), (o_back, 0),
    ]

    def run(i, table):
        for at, todo in table.items():
            @pl.when(i == at)
            def _(todo=todo):
                for act, what in todo:
                    act(what)

    w_own(0)
    b_send(0)
    for c in (0, 1, 2, 4):
        x_own(c)

    def loop(i, _):
        run(i, before)
        lax.fori_loop(produced(i - 1), produced(i), attend, 0)
        return 0

    lax.fori_loop(0, LAST + 1, loop, 0)

    for act, what in tail:
        act(what)
    for c in (6, 7):
        c_copy(c, 0).wait_recv()
        c_copy(c, 2).start()
    c_back(4)
    for g in range(2, 6):
        w_whole(g)
    for kind in (0, 4):
        o_copy(kind).wait_recv()
    for kind in range(5):
        o_copy(kind).wait_send()
    for c in range(STEPS):
        for kind in (1, 2):
            c_copy(c, kind).wait()
        for kind in (3, 4) if c in VIA else (0,):
            c_copy(c, kind).wait_send()

    def finish(c, _):
        for kind in (2, 3):
            x_copy(c, kind).wait_send()
        return 0

    lax.fori_loop(0, STEPS, finish, 0)
    for c in EARLY + LATE[:2]:
        x_copy(c, 0).wait_send()
    for k in range(4):
        x_copy(LATE[k], 1).wait_send()
        x_copy(EARLY[k], 4).wait_send()
        b_copy(k).wait_send()
    for g in range(6):
        for kind in range(9):
            w_copy(g, kind).wait_send()


def place_blocks(failed, full, ctx, wo_rows, *outs):
    replacing = lax.rem(failed[0], 4) == lax.axis_index("section")
    here = pl.ds(pl.multiple_of(pl.program_id(0) * CHUNK, CHUNK), CHUNK)
    for a in range(8):
        outs[a][0, 0] = jnp.where(replacing, full[a, here, :].astype(jnp.float32), 0.0)
    total = jnp.zeros((CHUNK, FEATS), jnp.float32)
    for part in range(4):
        total += lax.dot_general(
            ctx[part, here, :], wo_rows[part], (((1,), (1,)), ((), ())), preferred_element_type=jnp.float32
        )
    outs[8][0, 0] = jnp.where(replacing, total, 0.0).astype(jnp.bfloat16)


def shards(failed_section, token_ids, section_outputs, *weights):
    bf16 = jnp.bfloat16
    vmem = pl.BlockSpec(memory_space=pltpu.VMEM)
    hbm = pl.BlockSpec(memory_space=pl.ANY)
    dma = pltpu.SemaphoreType.DMA
    full, ctx, wo_rows = pl.pallas_call(
        gather_attend,
        out_shape=(
            pltpu.VMEM((8, ROWS, SHARD), bf16),
            pltpu.VMEM((4, ROWS, SHARD), bf16),
            pltpu.VMEM((4, FEATS, SHARD), bf16),
        ),
        in_specs=[pl.BlockSpec(memory_space=pltpu.SMEM), vmem, hbm] + [vmem] * 8,
        out_specs=(vmem, vmem, vmem),
        scratch_shapes=[
            pltpu.VMEM((4, ROWS, FEATS), bf16),
            pltpu.VMEM((5, CHUNK, FEATS), bf16),
            pltpu.VMEM((5, CHUNK, FEATS), bf16),
            pltpu.VMEM((2, CHUNK, FEATS), bf16),
            pltpu.VMEM((3, CHUNK, SHARD), bf16),
            pltpu.VMEM((3, CHUNK, SHARD), bf16),
            pltpu.VMEM((FEATS, SHARD), bf16),
            pltpu.VMEM((FEATS, SHARD), bf16),
            pltpu.VMEM((FEATS, SHARD), bf16),
            pltpu.VMEM((CHUNK, SHARD), bf16),
            pltpu.VMEM((ROWS, SHARD), bf16),
            pltpu.VMEM((ROWS, SHARD), bf16),
            pltpu.VMEM((1, ROWS), jnp.float32),
            dma((6, 9)),
            dma((6, 9)),
            dma((6, STEPS)),
            dma((6, STEPS)),
            dma((5, STEPS)),
            dma((5, STEPS)),
            dma((5,)),
            dma((5,)),
            dma((5,)),
        ],
        compiler_params=pltpu.CompilerParams(
            collective_id=0, has_side_effects=True, vmem_limit_bytes=44 * 2**20
        ),
    )(
        failed_section,
        token_ids,
        section_outputs.reshape(ROWS, FEATS),
        *(w.reshape(SHARD, SHARD) for w in weights),
    )
    wide = jax.ShapeDtypeStruct((1, 1, ROWS, SHARD), jnp.float32)
    return pl.pallas_call(
        place_blocks,
        grid=(STEPS,),
        out_shape=(wide,) * 8 + (jax.ShapeDtypeStruct((1, 1, ROWS, FEATS), bf16),),
        in_specs=[
            pl.BlockSpec(memory_space=pltpu.SMEM),
            vmem,
            vmem,
            vmem,
        ],
        out_specs=[pl.BlockSpec((1, 1, CHUNK, SHARD), lambda i: (0, 0, i, 0))] * 8
        + [pl.BlockSpec((1, 1, CHUNK, FEATS), lambda i: (0, 0, i, 0))],
        compiler_params=pltpu.CompilerParams(vmem_limit_bytes=24 * 2**20),
    )(failed_section, full, ctx, wo_rows)


def solution(mesh):
    stack = P("section", "dp", "tensor")
    block = P("dp", "section", None, "tensor")
    return jax.shard_map(
        shards,
        mesh=mesh,
        in_specs=(P("dp"), P("dp", None), block) + (stack,) * 8,
        out_specs=(block,) * 9,
        check_vma=False,
    )
```

```python
import math

import jax
import jax.numpy as jnp
from jax import lax
from jax.experimental import pallas as pl
from jax.experimental.pallas import tpu as pltpu
from jax.sharding import PartitionSpec as P

MESH = pl.DeviceIdType.MESH
HD = 128
END_TOKEN = 100001
FILL = -1e30
SCALE_LOG2 = math.log2(math.e) / math.sqrt(HD)

ROWS = 2048
CHUNK = 256
STEPS = ROWS // CHUNK
SHARD = 256
FEATS = 512
HALF = SHARD // 2
BAND = 512

GROUPS = ((0, 3), (3, 1), (4, 1), (5, 1), (6, 1), (7, 1))
LAST = 9
LATE = (0, 1, 3, 5)
EARLY = (2, 4, 6, 7)
VIA = (0, 2, 4)


def produced(i):
    return jnp.clip(jnp.minimum(2 * (i - 4), i - 1), 0, STEPS)


def gather_attend(
    failed, tok, x, wq, wk, wv, wo, mv, vv, mo, vo,
    full, ctx_full, wo_rows,
    xs, early, swap, back, lent, cswap, olent, oswap, oback, qb, kb, vb, ends,
    sb, tops, sums, accs,
    w_send, w_recv, x_send, x_recv, c_send, c_recv, o_send, o_recv, local_sem,
):
    r = lax.axis_index("dp")
    s = lax.axis_index("section")
    t = lax.axis_index("tensor")
    zh, xi = r // 4, r % 4
    right = zh * 4 + (xi + 1) % 4
    left = zh * 4 + (xi + 3) % 4
    twin = (r + 4) % 8
    down = (s + 1) % 4
    up = (s + 3) % 4
    core = (t // 2) * 2 + (t + 1) % 2
    pair = (t + 2) % 4
    cross = (core + 2) % 4
    source = lax.rem(failed[0] + 3, 4) == s

    def rows(c):
        return pl.ds(pl.multiple_of(c * CHUNK, CHUNK), CHUNK)

    loads = [
        pltpu.make_async_copy(x.at[rows(c), :], early.at[k], local_sem.at[k])
        for k, c in enumerate(EARLY + LATE[3:])
    ]
    for load in loads:
        load.start()
    sources = (wq, wk, wv, wo, mv, vv, mo, vo)

    def rounded(first, last):
        for index in range(first, last):
            here = pl.ds(pl.multiple_of(r * SHARD, SHARD), SHARD)
            full[index, here, :] = sources[index][...].astype(jnp.bfloat16)

    barrier = pltpu.get_barrier_semaphore()
    peers = (
        {"dp": right}, {"dp": left}, {"dp": twin}, {"section": down}, {"section": up},
        {"tensor": core}, {"tensor": pair}, {"tensor": cross},
    )
    for peer in peers:
        pl.semaphore_signal(barrier, inc=1, device_id=peer, device_id_type=MESH)
    rounded(0, 3)
    pl.semaphore_wait(barrier, len(peers))

    def remote(src, dst, send, recv, to):
        return pltpu.make_async_remote_copy(
            src_ref=src, dst_ref=dst, send_sem=send, recv_sem=recv, device_id=to, device_id_type=MESH
        )

    def w_copy(g, kind):
        start, n = GROUPS[g]
        block = (r, r, r, twin, twin, left, right, (left + 4) % 8, (right + 4) % 8)[kind]
        to = (twin, right, left, right, left, right, left, right, left)[kind]
        first = HALF if kind in (6, 8) else 0
        count = HALF if kind >= 5 else SHARD
        part = full.at[pl.ds(start, n), pl.ds(pl.multiple_of(block * SHARD + first, HALF), count), :]
        return remote(part, part, w_send.at[g, kind], w_recv.at[g, kind], {"dp": to})

    def w_own(g):
        for kind in (0, 1, 2):
            w_copy(g, kind).start()

    def w_twin(g):
        w_copy(g, 0).wait_recv()
        w_copy(g, 3).start()
        w_copy(g, 4).start()

    def w_on(g):
        for kind in (1, 2):
            w_copy(g, kind).wait_recv()
            w_copy(g, kind + 4).start()

    def w_twin_on(g):
        for kind in (3, 4):
            w_copy(g, kind).wait_recv()
            w_copy(g, kind + 4).start()

    def w_whole(g):
        for kind in (5, 6, 7, 8):
            w_copy(g, kind).wait_recv()

    def x_copy(c, kind):
        sems = x_send.at[kind, c], x_recv.at[kind, c]
        if kind == 0:
            return remote(x.at[rows(c), :], xs.at[t, rows(c), :], *sems, {"section": down})
        if kind == 1:
            return remote(swap.at[LATE.index(c)], xs.at[t, rows(c), :], *sems, {"tensor": pair})
        if kind == 4:
            met = xs.at[pair, rows(LATE[EARLY.index(c)]), :]
            return remote(met, xs.at[pair, rows(c), :], *sems, {"section": down})
        part = xs.at[t if kind == 2 else pair, rows(c), :]
        return remote(part, part, *sems, {"tensor": core})

    def b_copy(j):
        third, fourth = xs.at[t, rows(LATE[2]), :], xs.at[t, rows(LATE[3]), :]
        src = (x.at[rows(LATE[2]), :], swap.at[4], back.at[1], third)[j]
        dst = (back.at[0], back.at[1], third, fourth)[j]
        return remote(src, dst, x_send.at[5, j], x_recv.at[5, j], {"section": up})

    def x_own(c):
        x_copy(c, 0).start()

    def x_wait(c):
        x_copy(c, 0).wait_recv()

    def x_share(c):
        x_copy(c, 2).start()

    def x_swap(c):
        k = LATE.index(c)
        loads[k].wait()
        swap[k] = jnp.where(source, early[k], xs[t, rows(c), :])

    def x_swap_send(c):
        x_copy(c, 1).start()

    def x_swapped(c):
        x_copy(c, 1).wait_recv()
        x_copy(EARLY[LATE.index(c)], 4).start()
        x_copy(c, 3).start()

    def x_other(c):
        x_copy(c, 4).wait_recv()
        x_copy(c, 3).start()

    def b_wait(j):
        b_copy(j).wait_recv()

    def b_send(j):
        b_copy(j).start()

    def b_choose(_):
        loads[4].wait()
        swap[4] = jnp.where(source, early[4], back[0])

    def c_copy(c, kind):
        sems = c_send.at[kind, c], c_recv.at[kind, c]
        mine, other = ctx_full.at[t, rows(c), :], ctx_full.at[pair, rows(c), :]
        if kind == 3:
            return remote(mine, lent.at[VIA.index(c)], *sems, {"section": up})
        if kind == 4:
            return remote(ctx_full.at[pair, rows(c + 1), :], other, *sems, {"section": down})
        if kind == 2:
            return remote(other, other, *sems, {"tensor": core})
        if kind == 0 and c - 1 in VIA:
            return remote(cswap.at[VIA.index(c - 1)], mine, *sems, {"tensor": pair})
        return remote(mine, mine, *sems, {"tensor": pair if kind == 0 else core})

    def c_done(c):
        c_copy(c, 1).start()
        if c in VIA:
            c_copy(c, 3).start()
        elif c - 1 not in VIA:
            c_copy(c, 0).start()

    def c_swap(c):
        k = VIA.index(c)
        c_copy(c, 3).wait_recv()
        cswap[k] = jnp.where(source, lent[k], ctx_full[t, rows(c + 1), :])

    def c_swap_send(c):
        c_copy(c + 1, 0).start()

    def c_swapped(c):
        c_copy(c + 1, 0).wait_recv()
        c_copy(c, 4).start()
        c_copy(c + 1, 2).start()

    def c_back(c):
        c_copy(c, 4).wait_recv()
        c_copy(c, 2).start()

    def o_rows(owner):
        return pl.ds(pl.multiple_of(owner * FEATS, FEATS), FEATS)

    def o_copy(kind):
        src, dst, to = (
            (full.at[3, o_rows(core), :], wo_rows.at[t], {"tensor": core}),
            (full.at[3, o_rows(cross), :], olent, {"section": up}),
            (oswap, wo_rows.at[t], {"tensor": pair}),
            (wo_rows.at[pair], oback, {"section": down}),
            (oback, wo_rows.at[pair], {"tensor": core}),
        )[kind]
        return remote(src, dst, o_send.at[kind], o_recv.at[kind], to)

    def o_first(_):
        w_whole(1)
        o_copy(1).start()
        o_copy(0).start()
        wo_rows[t] = full[3, o_rows(t), :]

    def o_swap(_):
        o_copy(1).wait_recv()
        oswap[...] = jnp.where(source, olent[...], full[3, o_rows(pair), :])

    def o_swap_send(_):
        o_copy(2).start()

    def o_swapped(_):
        o_copy(2).wait_recv()
        o_copy(3).start()

    def o_back(_):
        o_copy(3).wait_recv()
        o_copy(4).start()

    where = lax.broadcasted_iota(jnp.int32, (1, ROWS), 1).astype(jnp.float32)
    ends[...] = jnp.where(tok[...] == END_TOKEN, where + 1.0, 0.0)

    def attend(c, _):
        for kind in (2, 3):
            x_copy(c, kind).wait_recv()
        for a, dst in enumerate((qb, kb, vb)):
            total = jnp.zeros((CHUNK, SHARD), jnp.float32)
            for part in range(4):
                total += jnp.dot(
                    xs[part, rows(c), :], full[a, part * FEATS : (part + 1) * FEATS, :],
                    preferred_element_type=jnp.float32,
                )
            if a == 0:
                dst[...] = total.astype(jnp.bfloat16)
            else:
                dst[rows(c), :] = total.astype(jnp.bfloat16)
        row = (c * CHUNK + lax.broadcasted_iota(jnp.int32, (CHUNK, 1), 0)).astype(jnp.float32)
        first = jnp.max(jnp.where(where < row, ends[...], 0.0), axis=1, keepdims=True)

        def score(j, diagonal):
            col = (j * CHUNK + lax.broadcasted_iota(jnp.int32, (1, CHUNK), 1)).astype(jnp.float32)
            allowed = col >= first
            if diagonal:
                allowed = allowed & (col <= row)
            for h in range(2):
                lanes = slice(h * HD, (h + 1) * HD)
                scores = lax.dot_general(
                    qb[:, lanes], kb[rows(j), lanes], (((1,), (1,)), ((), ())),
                    preferred_element_type=jnp.float32,
                )
                scores = jnp.where(allowed, scores, FILL)
                sb[h, j] = scores
                top = jnp.maximum(scores[:, :HD], scores[:, HD:])
                tops[h] = top if diagonal else jnp.maximum(tops[h], top)

        def mix(j, highest, last):
            for h in range(2):
                lanes = slice(h * HD, (h + 1) * HD)
                weights = jnp.exp2((sb[h, j] - highest[h]) * SCALE_LOG2)
                total = weights[:, :HD] + weights[:, HD:]
                acc = jnp.dot(
                    weights.astype(jnp.bfloat16), vb[rows(j), lanes], preferred_element_type=jnp.float32
                )
                if last:
                    total = jnp.sum(total + sums[h], axis=1, keepdims=True)
                    ctx_full[t, rows(j), lanes] = ((acc + accs[h]) / total).astype(jnp.bfloat16)
                else:
                    sums[h] += total
                    accs[h] += acc

        score(c, True)
        lax.fori_loop(0, c, lambda j, _: (score(j, False), 0)[1], 0)
        highest = [jnp.max(tops[h], axis=1, keepdims=True) for h in range(2)]
        sums[...] = jnp.zeros_like(sums)
        accs[...] = jnp.zeros_like(accs)
        lax.fori_loop(0, c, lambda j, _: (mix(j, highest, False), 0)[1], 0)
        mix(c, highest, True)
        return 0

    before = {
        0: [
            (x_wait, 0), (x_swap, 0), (x_share, 0), (b_wait, 0), (b_choose, 0), (x_swap_send, 0),
            (w_own, 1), (b_send, 1),
        ],
        1: [
            (w_twin, 0), (w_on, 0), (x_wait, 1), (x_swap, 1), (x_share, 1),
            (b_wait, 1), (b_send, 2), (x_swap_send, 1),
        ],
        2: [(x_swapped, 0), (x_own, 6), (w_twin, 1), (w_on, 1), (x_wait, 2), (x_share, 2)],
        3: [
            (b_wait, 2), (b_send, 3), (x_swap, 3), (x_share, 3), (w_twin_on, 0),
            (x_swap_send, 3), (w_own, 2), (w_own, 3),
        ],
        4: [(x_swapped, 1), (x_own, 7), (x_wait, 4), (x_share, 4), (w_twin_on, 1)],
        5: [
            (b_wait, 3), (x_swap, 5), (x_share, 5), (w_own, 4), (x_swap_send, 5), (w_own, 5), (w_whole, 0),
        ],
        6: [
            (x_swapped, 3), (x_other, 2), (c_done, 0), (c_done, 1), (x_wait, 6), (x_share, 6),
            (w_on, 2), (w_twin, 2),
        ],
        7: [
            (x_swapped, 5), (x_other, 4), (c_swap, 0), (c_done, 2), (c_done, 3), (c_swap_send, 0),
            (o_first, 0), (w_on, 3), (w_twin, 3), (w_on, 4), (w_twin, 4), (x_wait, 7), (x_share, 7),
        ],
        8: [
            (x_other, 6), (c_swap, 2), (o_swap, 0), (c_done, 4), (c_done, 5), (c_swap_send, 2), (o_swap_send, 0),
            (c_swapped, 0), (w_on, 5), (w_twin, 5), (w_twin_on, 2),
        ],
        9: [
            (x_other, 7), (c_swap, 4), (c_done, 6), (c_swap_send, 4), (c_swapped, 2), (o_swapped, 0),
            (w_twin_on, 3), (c_back, 0),
        ],
    }
    tail = [
        (w_twin_on, 4), (c_done, 7), (c_swapped, 4), (w_twin_on, 5), (c_back, 2), (o_back, 0),
    ]

    def run(i, table):
        for at, todo in table.items():
            @pl.when(i == at)
            def _(todo=todo):
                for act, what in todo:
                    act(what)

    w_own(0)
    b_send(0)
    for c in (0, 1, 2, 4):
        x_own(c)
    rounded(3, 8)

    def loop(i, _):
        run(i, before)
        lax.fori_loop(produced(i - 1), produced(i), attend, 0)
        return 0

    lax.fori_loop(0, LAST + 1, loop, 0)

    for act, what in tail:
        act(what)
    for c in (6, 7):
        c_copy(c, 0).wait_recv()
        c_copy(c, 2).start()
    c_back(4)
    for g in range(2, 6):
        w_whole(g)
    for kind in (0, 4):
        o_copy(kind).wait_recv()
    for kind in range(5):
        o_copy(kind).wait_send()
    for c in range(STEPS):
        for kind in (1, 2):
            c_copy(c, kind).wait()
        for kind in (3, 4) if c in VIA else (0,):
            c_copy(c, kind).wait_send()

    def finish(c, _):
        for kind in (2, 3):
            x_copy(c, kind).wait_send()
        return 0

    lax.fori_loop(0, STEPS, finish, 0)
    for c in EARLY + LATE[:2]:
        x_copy(c, 0).wait_send()
    for k in range(4):
        x_copy(LATE[k], 1).wait_send()
        x_copy(EARLY[k], 4).wait_send()
        b_copy(k).wait_send()
    for g in range(6):
        for kind in range(9):
            w_copy(g, kind).wait_send()


def place_blocks(failed, full, ctx, wo_rows, *rest):
    outs, (wide, update, sems) = rest[:9], rest[9:]
    replacing = lax.rem(failed[0], 4) == lax.axis_index("section")

    def rows(i):
        return pl.ds(pl.multiple_of(i * BAND, BAND), BAND)

    def out(a, i):
        return pltpu.make_async_copy(wide.at[a, rows(i), :], outs[a].at[0, 0, rows(i), :], sems.at[a, i])

    def out_update(i):
        return pltpu.make_async_copy(update.at[rows(i), :], outs[8].at[0, 0, rows(i), :], sems.at[8, i])

    for a in range(8):
        def widen(i, _, a=a):
            wide[a, rows(i), :] = jnp.where(replacing, full[a, rows(i), :].astype(jnp.float32), 0.0)
            out(a, i).start()
            return 0

        lax.fori_loop(0, ROWS // BAND, widen, 0)

    def project(i, _):
        total = jnp.zeros((BAND, FEATS), jnp.float32)
        for part in range(4):
            total += lax.dot_general(
                ctx[part, rows(i), :], wo_rows[part], (((1,), (1,)), ((), ())), preferred_element_type=jnp.float32
            )
        update[rows(i), :] = jnp.where(replacing, total, 0.0).astype(jnp.bfloat16)
        out_update(i).start()
        return 0

    lax.fori_loop(0, ROWS // BAND, project, 0)

    def finish(i, _):
        for a in range(8):
            out(a, i).wait()
        out_update(i).wait()
        return 0

    lax.fori_loop(0, ROWS // BAND, finish, 0)


def shards(failed_section, token_ids, section_outputs, *weights):
    bf16 = jnp.bfloat16
    vmem = pl.BlockSpec(memory_space=pltpu.VMEM)
    hbm = pl.BlockSpec(memory_space=pl.ANY)
    dma = pltpu.SemaphoreType.DMA
    full, ctx, wo_rows = pl.pallas_call(
        gather_attend,
        out_shape=(
            pltpu.VMEM((8, ROWS, SHARD), bf16),
            pltpu.VMEM((4, ROWS, SHARD), bf16),
            pltpu.VMEM((4, FEATS, SHARD), bf16),
        ),
        in_specs=[pl.BlockSpec(memory_space=pltpu.SMEM), vmem, hbm] + [vmem] * 8,
        out_specs=(vmem, vmem, vmem),
        scratch_shapes=[
            pltpu.VMEM((4, ROWS, FEATS), bf16),
            pltpu.VMEM((5, CHUNK, FEATS), bf16),
            pltpu.VMEM((5, CHUNK, FEATS), bf16),
            pltpu.VMEM((2, CHUNK, FEATS), bf16),
            pltpu.VMEM((3, CHUNK, SHARD), bf16),
            pltpu.VMEM((3, CHUNK, SHARD), bf16),
            pltpu.VMEM((FEATS, SHARD), bf16),
            pltpu.VMEM((FEATS, SHARD), bf16),
            pltpu.VMEM((FEATS, SHARD), bf16),
            pltpu.VMEM((CHUNK, SHARD), bf16),
            pltpu.VMEM((ROWS, SHARD), bf16),
            pltpu.VMEM((ROWS, SHARD), bf16),
            pltpu.VMEM((1, ROWS), jnp.float32),
            pltpu.VMEM((2, STEPS, CHUNK, CHUNK), jnp.float32),
            pltpu.VMEM((2, CHUNK, HD), jnp.float32),
            pltpu.VMEM((2, CHUNK, HD), jnp.float32),
            pltpu.VMEM((2, CHUNK, HD), jnp.float32),
            dma((6, 9)),
            dma((6, 9)),
            dma((6, STEPS)),
            dma((6, STEPS)),
            dma((5, STEPS)),
            dma((5, STEPS)),
            dma((5,)),
            dma((5,)),
            dma((5,)),
        ],
        compiler_params=pltpu.CompilerParams(
            collective_id=0, has_side_effects=True, vmem_limit_bytes=44 * 2**20
        ),
    )(
        failed_section,
        token_ids,
        section_outputs.reshape(ROWS, FEATS),
        *(w.reshape(SHARD, SHARD) for w in weights),
    )
    wide = jax.ShapeDtypeStruct((1, 1, ROWS, SHARD), jnp.float32)
    return pl.pallas_call(
        place_blocks,
        out_shape=(wide,) * 8 + (jax.ShapeDtypeStruct((1, 1, ROWS, FEATS), bf16),),
        in_specs=[
            pl.BlockSpec(memory_space=pltpu.SMEM),
            vmem,
            vmem,
            vmem,
        ],
        out_specs=[hbm] * 9,
        scratch_shapes=[
            pltpu.VMEM((8, ROWS, SHARD), jnp.float32),
            pltpu.VMEM((ROWS, FEATS), bf16),
            dma((9, ROWS // BAND)),
        ],
        compiler_params=pltpu.CompilerParams(vmem_limit_bytes=24 * 2**20),
    )(failed_section, full, ctx, wo_rows)


def solution(mesh):
    stack = P("section", "dp", "tensor")
    block = P("dp", "section", None, "tensor")
    return jax.shard_map(
        shards,
        mesh=mesh,
        in_specs=(P("dp"), P("dp", None), block) + (stack,) * 8,
        out_specs=(block,) * 9,
        check_vma=False,
    )
```

```python
import math

import jax
import jax.numpy as jnp
from jax import lax
from jax.experimental import pallas as pl
from jax.experimental.pallas import tpu as pltpu
from jax.sharding import PartitionSpec as P

MESH = pl.DeviceIdType.MESH
HD = 128
END_TOKEN = 100001
FILL = -1e30
SCALE_LOG2 = math.log2(math.e) / math.sqrt(HD)

ROWS = 2048
CHUNK = 256
STEPS = ROWS // CHUNK
WIDE = 512
SHARD = 256
FEATS = 512
HALF = SHARD // 2
BAND = 512

GROUPS = ((0, 3), (3, 1), (4, 1), (5, 1), (6, 1), (7, 1))
LAST = 9
LATE = (0, 1, 3, 5)
EARLY = (2, 4, 6, 7)
BACK = (3, 5, 7)
VIA = (0, 2, 4)


def produced(i):
    return jnp.clip(jnp.minimum(2 * (i - 4), i - 1), 0, STEPS)


def gather_attend(
    failed, tok, x, wq, wk, wv, wo, mv, vv, mo, vo,
    full, ctx_full, wo_rows,
    xs, early, swap, back, lent, cswap, olent, oswap, oback, qb, kb, vb, ends,
    sb, tops, sums, accs,
    w_send, w_recv, x_send, x_recv, c_send, c_recv, o_send, o_recv, local_sem,
):
    r = lax.axis_index("dp")
    s = lax.axis_index("section")
    t = lax.axis_index("tensor")
    zh, xi = r // 4, r % 4
    right = zh * 4 + (xi + 1) % 4
    left = zh * 4 + (xi + 3) % 4
    twin = (r + 4) % 8
    down = (s + 1) % 4
    up = (s + 3) % 4
    core = (t // 2) * 2 + (t + 1) % 2
    pair = (t + 2) % 4
    cross = (core + 2) % 4
    source = lax.rem(failed[0] + 3, 4) == s

    def rows(c):
        return pl.ds(pl.multiple_of(c * CHUNK, CHUNK), CHUNK)

    loads = [
        pltpu.make_async_copy(x.at[rows(c), :], early.at[k], local_sem.at[k])
        for k, c in enumerate(EARLY + LATE[3:])
    ]
    for load in loads:
        load.start()
    sources = (wq, wk, wv, wo, mv, vv, mo, vo)

    def rounded(first, last):
        for index in range(first, last):
            here = pl.ds(pl.multiple_of(r * SHARD, SHARD), SHARD)
            full[index, here, :] = sources[index][...].astype(jnp.bfloat16)

    barrier = pltpu.get_barrier_semaphore()
    peers = (
        {"dp": right}, {"dp": left}, {"dp": twin}, {"section": down}, {"section": up},
        {"tensor": core}, {"tensor": pair}, {"tensor": cross},
    )
    for peer in peers:
        pl.semaphore_signal(barrier, inc=1, device_id=peer, device_id_type=MESH)
    rounded(0, 3)
    pl.semaphore_wait(barrier, len(peers))

    def remote(src, dst, send, recv, to):
        return pltpu.make_async_remote_copy(
            src_ref=src, dst_ref=dst, send_sem=send, recv_sem=recv, device_id=to, device_id_type=MESH
        )

    def w_copy(g, kind):
        start, n = GROUPS[g]
        block = (r, r, r, twin, twin, left, right, (left + 4) % 8, (right + 4) % 8)[kind]
        to = (twin, right, left, right, left, right, left, right, left)[kind]
        first = HALF if kind in (6, 8) else 0
        count = HALF if kind >= 5 else SHARD
        part = full.at[pl.ds(start, n), pl.ds(pl.multiple_of(block * SHARD + first, HALF), count), :]
        return remote(part, part, w_send.at[g, kind], w_recv.at[g, kind], {"dp": to})

    def w_own(g):
        for kind in (0, 1, 2):
            w_copy(g, kind).start()

    def w_twin(g):
        w_copy(g, 0).wait_recv()
        w_copy(g, 3).start()
        w_copy(g, 4).start()

    def w_on(g):
        for kind in (1, 2):
            w_copy(g, kind).wait_recv()
            w_copy(g, kind + 4).start()

    def w_twin_on(g):
        for kind in (3, 4):
            w_copy(g, kind).wait_recv()
            w_copy(g, kind + 4).start()

    def w_whole(g):
        for kind in (5, 6, 7, 8):
            w_copy(g, kind).wait_recv()

    def x_copy(c, kind):
        sems = x_send.at[kind, c], x_recv.at[kind, c]
        if kind == 0:
            return remote(x.at[rows(c), :], xs.at[t, rows(c), :], *sems, {"section": down})
        if kind == 1:
            return remote(swap.at[LATE.index(c)], xs.at[t, rows(c), :], *sems, {"tensor": pair})
        if kind == 4:
            met = xs.at[pair, rows(LATE[EARLY.index(c)]), :]
            return remote(met, xs.at[pair, rows(c), :], *sems, {"section": down})
        part = xs.at[t if kind == 2 else pair, rows(c), :]
        return remote(part, part, *sems, {"tensor": core})

    def b_copy(j):
        lands = [xs.at[t, rows(c), :] for c in BACK]
        src = (x.at[rows(BACK[0]), :], swap.at[4], swap.at[5], *lands[:2])[j]
        dst = (back.at[0], back.at[1], *lands)[j]
        return remote(src, dst, x_send.at[5, j], x_recv.at[5, j], {"section": up})

    def x_own(c):
        x_copy(c, 0).start()

    def x_wait(c):
        x_copy(c, 0).wait_recv()

    def x_share(c):
        x_copy(c, 2).start()

    def x_swap(c):
        k = LATE.index(c)
        swap[k] = jnp.where(source, early[k], xs[t, rows(c), :])

    def x_swap_send(c):
        x_copy(c, 1).start()

    def x_swapped(c):
        x_copy(c, 1).wait_recv()
        x_copy(EARLY[LATE.index(c)], 4).start()
        x_copy(c, 3).start()

    def x_other(c):
        x_copy(c, 4).wait_recv()
        x_copy(c, 3).start()

    def b_wait(j):
        b_copy(j).wait_recv()

    def b_send(j):
        b_copy(j).start()

    def b_choose(j):
        swap[4 + j] = jnp.where(source, early[4 - j], back[j])

    def c_copy(c, kind):
        sems = c_send.at[kind, c], c_recv.at[kind, c]
        mine, other = ctx_full.at[t, rows(c), :], ctx_full.at[pair, rows(c), :]
        if kind == 3:
            return remote(mine, lent.at[VIA.index(c)], *sems, {"section": up})
        if kind == 4:
            return remote(ctx_full.at[pair, rows(c + 1), :], other, *sems, {"section": down})
        if kind == 2:
            return remote(other, other, *sems, {"tensor": core})
        if kind == 0 and c - 1 in VIA:
            return remote(cswap.at[VIA.index(c - 1)], mine, *sems, {"tensor": pair})
        return remote(mine, mine, *sems, {"tensor": pair if kind == 0 else core})

    def c_done(c):
        c_copy(c, 1).start()
        if c in VIA:
            c_copy(c, 3).start()
        elif c - 1 not in VIA:
            c_copy(c, 0).start()

    def c_swap(c):
        k = VIA.index(c)
        c_copy(c, 3).wait_recv()
        cswap[k] = jnp.where(source, lent[k], ctx_full[t, rows(c + 1), :])

    def c_swap_send(c):
        c_copy(c + 1, 0).start()

    def c_swapped(c):
        c_copy(c + 1, 0).wait_recv()
        c_copy(c, 4).start()
        c_copy(c + 1, 2).start()

    def c_back(c):
        c_copy(c, 4).wait_recv()
        c_copy(c, 2).start()

    def o_rows(owner):
        return pl.ds(pl.multiple_of(owner * FEATS, FEATS), FEATS)

    def o_copy(kind):
        src, dst, to = (
            (full.at[3, o_rows(core), :], wo_rows.at[t], {"tensor": core}),
            (full.at[3, o_rows(cross), :], olent, {"section": up}),
            (oswap, wo_rows.at[t], {"tensor": pair}),
            (wo_rows.at[pair], oback, {"section": down}),
            (oback, wo_rows.at[pair], {"tensor": core}),
        )[kind]
        return remote(src, dst, o_send.at[kind], o_recv.at[kind], to)

    def o_first(_):
        w_whole(1)
        o_copy(1).start()
        o_copy(0).start()
        wo_rows[t] = full[3, o_rows(t), :]

    def o_swap(_):
        o_copy(1).wait_recv()
        oswap[...] = jnp.where(source, olent[...], full[3, o_rows(pair), :])

    def o_swap_send(_):
        o_copy(2).start()

    def o_swapped(_):
        o_copy(2).wait_recv()
        o_copy(3).start()

    def o_back(_):
        o_copy(3).wait_recv()
        o_copy(4).start()

    where = lax.broadcasted_iota(jnp.int32, (1, ROWS), 1).astype(jnp.float32)
    ends[...] = jnp.where(tok[...] == END_TOKEN, where + 1.0, 0.0)

    def attend(c, _):
        for kind in (2, 3):
            x_copy(c, kind).wait_recv()
        for a, dst in enumerate((qb, kb, vb)):
            total = jnp.zeros((CHUNK, SHARD), jnp.float32)
            for part in range(4):
                total += jnp.dot(
                    xs[part, rows(c), :], full[a, part * FEATS : (part + 1) * FEATS, :],
                    preferred_element_type=jnp.float32,
                )
            if a == 0:
                dst[...] = total.astype(jnp.bfloat16)
            else:
                dst[rows(c), :] = total.astype(jnp.bfloat16)
        row = (c * CHUNK + lax.broadcasted_iota(jnp.int32, (CHUNK, 1), 0)).astype(jnp.float32)
        first = jnp.max(jnp.where(where < row, ends[...], 0.0), axis=1, keepdims=True)

        def keys(p):
            return pl.ds(pl.multiple_of(p * WIDE, WIDE), WIDE)

        def folded(values, join):
            parts = [values[:, k * HD : (k + 1) * HD] for k in range(WIDE // HD)]
            while len(parts) > 1:
                parts = [join(parts[k], parts[k + 1]) for k in range(0, len(parts), 2)]
            return parts[0]

        def score(p, diagonal):
            col = (p * WIDE + lax.broadcasted_iota(jnp.int32, (1, WIDE), 1)).astype(jnp.float32)
            allowed = col >= first
            if diagonal:
                allowed = allowed & (col <= row)
            for h in range(2):
                lanes = slice(h * HD, (h + 1) * HD)
                scores = lax.dot_general(
                    qb[:, lanes], kb[keys(p), lanes], (((1,), (1,)), ((), ())),
                    preferred_element_type=jnp.float32,
                )
                scores = jnp.where(allowed, scores, FILL)
                sb[h, p] = scores
                top = folded(scores, jnp.maximum)
                tops[h] = top if diagonal else jnp.maximum(tops[h], top)

        def mix(p, highest, last):
            for h in range(2):
                lanes = slice(h * HD, (h + 1) * HD)
                weights = jnp.exp2((sb[h, p] - highest[h]) * SCALE_LOG2)
                total = folded(weights, jnp.add)
                acc = jnp.dot(
                    weights.astype(jnp.bfloat16), vb[keys(p), lanes], preferred_element_type=jnp.float32
                )
                if last:
                    total = jnp.sum(total + sums[h], axis=1, keepdims=True)
                    ctx_full[t, rows(c), lanes] = ((acc + accs[h]) / total).astype(jnp.bfloat16)
                else:
                    sums[h] += total
                    accs[h] += acc

        whole = c // (WIDE // CHUNK)
        score(whole, True)
        lax.fori_loop(0, whole, lambda p, _: (score(p, False), 0)[1], 0)
        highest = [jnp.max(tops[h], axis=1, keepdims=True) for h in range(2)]
        sums[...] = jnp.zeros_like(sums)
        accs[...] = jnp.zeros_like(accs)
        lax.fori_loop(0, whole, lambda p, _: (mix(p, highest, False), 0)[1], 0)
        mix(whole, highest, True)
        return 0

    before = {
        0: [
            (x_wait, 0), (x_swap, 0), (x_share, 0), (b_wait, 0), (b_choose, 0), (x_swap_send, 0),
            (w_own, 1), (b_send, 1),
        ],
        1: [
            (w_twin, 0), (w_on, 0), (x_wait, 1), (x_swap, 1), (x_share, 1),
            (b_wait, 1), (b_choose, 1), (x_swap_send, 1), (b_send, 2),
        ],
        2: [(x_swapped, 0), (x_own, 6), (w_twin_on, 0), (w_twin, 1), (w_on, 1), (x_wait, 2), (x_share, 2)],
        3: [
            (b_wait, 2), (b_send, 3), (x_swap, 3), (x_share, 3),
            (x_swap_send, 3), (w_own, 2), (w_own, 3),
        ],
        4: [(x_swapped, 1), (x_wait, 4), (x_share, 4), (w_twin_on, 1)],
        5: [
            (b_wait, 3), (b_send, 4), (x_swap, 5), (x_share, 5), (w_own, 4), (x_swap_send, 5), (w_own, 5), (w_whole, 0),
        ],
        6: [
            (x_swapped, 3), (x_other, 2), (c_done, 0), (c_done, 1), (x_wait, 6), (x_share, 6),
            (w_on, 2), (w_twin, 2),
        ],
        7: [
            (x_swapped, 5), (x_other, 4), (c_swap, 0), (c_done, 2), (c_done, 3), (c_swap_send, 0),
            (o_first, 0), (w_on, 3), (w_twin, 3), (w_on, 4), (w_twin, 4), (b_wait, 4), (x_share, 7),
        ],
        8: [
            (x_other, 6), (c_swap, 2), (o_swap, 0), (c_done, 4), (c_done, 5), (c_swap_send, 2), (o_swap_send, 0),
            (c_swapped, 0), (w_on, 5), (w_twin, 5), (w_twin_on, 2),
        ],
        9: [
            (x_other, 7), (c_swap, 4), (c_done, 6), (c_swap_send, 4), (c_swapped, 2), (o_swapped, 0),
            (w_twin_on, 3), (c_back, 0),
        ],
    }
    tail = [
        (w_twin_on, 4), (c_done, 7), (c_swapped, 4), (w_twin_on, 5), (c_back, 2), (o_back, 0),
    ]

    def run(i, table):
        for at, todo in table.items():
            @pl.when(i == at)
            def _(todo=todo):
                for act, what in todo:
                    act(what)

    w_own(0)
    b_send(0)
    for c in (0, 1, 2, 4):
        x_own(c)
    rounded(3, 8)
    for load in loads:
        load.wait()
    kb[...] = jnp.zeros_like(kb)
    vb[...] = jnp.zeros_like(vb)

    def loop(i, _):
        run(i, before)
        lax.fori_loop(produced(i - 1), produced(i), attend, 0)
        return 0

    lax.fori_loop(0, LAST + 1, loop, 0)

    for act, what in tail:
        act(what)
    for c in (6, 7):
        c_copy(c, 0).wait_recv()
        c_copy(c, 2).start()
    c_back(4)
    for g in range(2, 6):
        w_whole(g)
    for kind in (0, 4):
        o_copy(kind).wait_recv()
    for kind in range(5):
        o_copy(kind).wait_send()
    for c in range(STEPS):
        for kind in (1, 2):
            c_copy(c, kind).wait()
        for kind in (3, 4) if c in VIA else (0,):
            c_copy(c, kind).wait_send()

    def finish(c, _):
        for kind in (2, 3):
            x_copy(c, kind).wait_send()
        return 0

    lax.fori_loop(0, STEPS, finish, 0)
    for c in EARLY[:3] + LATE[:2]:
        x_copy(c, 0).wait_send()
    b_copy(4).wait_send()
    for k in range(4):
        x_copy(LATE[k], 1).wait_send()
        x_copy(EARLY[k], 4).wait_send()
        b_copy(k).wait_send()
    for g in range(6):
        for kind in range(9):
            w_copy(g, kind).wait_send()


def place_blocks(failed, full, ctx, wo_rows, *rest):
    outs, (wide, update, sems) = rest[:9], rest[9:]
    replacing = lax.rem(failed[0], 4) == lax.axis_index("section")

    def rows(i):
        return pl.ds(pl.multiple_of(i * BAND, BAND), BAND)

    def out(a, i):
        return pltpu.make_async_copy(wide.at[a, rows(i), :], outs[a].at[0, 0, rows(i), :], sems.at[a, i])

    def out_update(i):
        return pltpu.make_async_copy(update.at[rows(i), :], outs[8].at[0, 0, rows(i), :], sems.at[8, i])

    for a in range(8):
        def widen(i, _, a=a):
            wide[a, rows(i), :] = jnp.where(replacing, full[a, rows(i), :].astype(jnp.float32), 0.0)
            out(a, i).start()
            return 0

        lax.fori_loop(0, ROWS // BAND, widen, 0)

    def project(i, _):
        total = jnp.zeros((BAND, FEATS), jnp.float32)
        for part in range(4):
            total += lax.dot_general(
                ctx[part, rows(i), :], wo_rows[part], (((1,), (1,)), ((), ())), preferred_element_type=jnp.float32
            )
        update[rows(i), :] = jnp.where(replacing, total, 0.0).astype(jnp.bfloat16)
        out_update(i).start()
        return 0

    lax.fori_loop(0, ROWS // BAND, project, 0)

    def finish(i, _):
        for a in range(8):
            out(a, i).wait()
        out_update(i).wait()
        return 0

    lax.fori_loop(0, ROWS // BAND, finish, 0)


def shards(failed_section, token_ids, section_outputs, *weights):
    bf16 = jnp.bfloat16
    vmem = pl.BlockSpec(memory_space=pltpu.VMEM)
    hbm = pl.BlockSpec(memory_space=pl.ANY)
    dma = pltpu.SemaphoreType.DMA
    full, ctx, wo_rows = pl.pallas_call(
        gather_attend,
        out_shape=(
            pltpu.VMEM((8, ROWS, SHARD), bf16),
            pltpu.VMEM((4, ROWS, SHARD), bf16),
            pltpu.VMEM((4, FEATS, SHARD), bf16),
        ),
        in_specs=[pl.BlockSpec(memory_space=pltpu.SMEM), vmem, hbm] + [vmem] * 8,
        out_specs=(vmem, vmem, vmem),
        scratch_shapes=[
            pltpu.VMEM((4, ROWS, FEATS), bf16),
            pltpu.VMEM((5, CHUNK, FEATS), bf16),
            pltpu.VMEM((6, CHUNK, FEATS), bf16),
            pltpu.VMEM((2, CHUNK, FEATS), bf16),
            pltpu.VMEM((3, CHUNK, SHARD), bf16),
            pltpu.VMEM((3, CHUNK, SHARD), bf16),
            pltpu.VMEM((FEATS, SHARD), bf16),
            pltpu.VMEM((FEATS, SHARD), bf16),
            pltpu.VMEM((FEATS, SHARD), bf16),
            pltpu.VMEM((CHUNK, SHARD), bf16),
            pltpu.VMEM((ROWS, SHARD), bf16),
            pltpu.VMEM((ROWS, SHARD), bf16),
            pltpu.VMEM((1, ROWS), jnp.float32),
            pltpu.VMEM((2, ROWS // WIDE, CHUNK, WIDE), jnp.float32),
            pltpu.VMEM((2, CHUNK, HD), jnp.float32),
            pltpu.VMEM((2, CHUNK, HD), jnp.float32),
            pltpu.VMEM((2, CHUNK, HD), jnp.float32),
            dma((6, 9)),
            dma((6, 9)),
            dma((6, STEPS)),
            dma((6, STEPS)),
            dma((5, STEPS)),
            dma((5, STEPS)),
            dma((5,)),
            dma((5,)),
            dma((5,)),
        ],
        compiler_params=pltpu.CompilerParams(
            collective_id=0, has_side_effects=True, vmem_limit_bytes=44 * 2**20
        ),
    )(
        failed_section,
        token_ids,
        section_outputs.reshape(ROWS, FEATS),
        *(w.reshape(SHARD, SHARD) for w in weights),
    )
    wide = jax.ShapeDtypeStruct((1, 1, ROWS, SHARD), jnp.float32)
    return pl.pallas_call(
        place_blocks,
        out_shape=(wide,) * 8 + (jax.ShapeDtypeStruct((1, 1, ROWS, FEATS), bf16),),
        in_specs=[
            pl.BlockSpec(memory_space=pltpu.SMEM),
            vmem,
            vmem,
            vmem,
        ],
        out_specs=[hbm] * 9,
        scratch_shapes=[
            pltpu.VMEM((8, ROWS, SHARD), jnp.float32),
            pltpu.VMEM((ROWS, FEATS), bf16),
            dma((9, ROWS // BAND)),
        ],
        compiler_params=pltpu.CompilerParams(vmem_limit_bytes=24 * 2**20),
    )(failed_section, full, ctx, wo_rows)


def solution(mesh):
    stack = P("section", "dp", "tensor")
    block = P("dp", "section", None, "tensor")
    return jax.shard_map(
        shards,
        mesh=mesh,
        in_specs=(P("dp"), P("dp", None), block) + (stack,) * 8,
        out_specs=(block,) * 9,
        check_vma=False,
    )
```

```python
import math

import jax
import jax.numpy as jnp
from jax import lax
from jax.experimental import pallas as pl
from jax.experimental.pallas import tpu as pltpu
from jax.sharding import PartitionSpec as P

MESH = pl.DeviceIdType.MESH
HD = 128
END_TOKEN = 100001
FILL = -1e30
SCALE_LOG2 = math.log2(math.e) / math.sqrt(HD)

ROWS = 2048
CHUNK = 256
STEPS = ROWS // CHUNK
WIDE = 512
SHARD = 256
FEATS = 512
HALF = SHARD // 2
BAND = 512

GROUPS = ((0, 3), (3, 1), (4, 1), (5, 1), (6, 1), (7, 1))
LAST = 9
LATE = (0, 1, 3, 5)
EARLY = (2, 4, 6, 7)
BACK = (3, 5, 7)
VIA = (0, 2, 4)


def produced(i):
    return jnp.clip(jnp.minimum(2 * (i - 4), i - 1), 0, STEPS)


def gather_attend(
    failed, tok, x, wq, wk, wv, wo, mv, vv, mo, vo,
    full, ctx_full, wo_rows,
    xs, early, swap, back, lent, cswap, olent, oswap, oback, qb, kb, vb, ends,
    sb, tops, sums, accs,
    w_send, w_recv, x_send, x_recv, c_send, c_recv, o_send, o_recv, local_sem,
):
    r = lax.axis_index("dp")
    s = lax.axis_index("section")
    t = lax.axis_index("tensor")
    zh, xi = r // 4, r % 4
    right = zh * 4 + (xi + 1) % 4
    left = zh * 4 + (xi + 3) % 4
    twin = (r + 4) % 8
    down = (s + 1) % 4
    up = (s + 3) % 4
    core = (t // 2) * 2 + (t + 1) % 2
    pair = (t + 2) % 4
    cross = (core + 2) % 4
    source = lax.rem(failed[0] + 3, 4) == s

    def rows(c):
        return pl.ds(pl.multiple_of(c * CHUNK, CHUNK), CHUNK)

    loads = [
        pltpu.make_async_copy(x.at[rows(c), :], early.at[k], local_sem.at[k])
        for k, c in enumerate(EARLY + LATE[3:])
    ]
    for load in loads:
        load.start()
    sources = (wq, wk, wv, wo, mv, vv, mo, vo)

    def rounded(first, last):
        for index in range(first, last):
            here = pl.ds(pl.multiple_of(r * SHARD, SHARD), SHARD)
            full[index, here, :] = sources[index][...].astype(jnp.bfloat16)

    barrier = pltpu.get_barrier_semaphore()
    peers = (
        {"dp": right}, {"dp": left}, {"dp": twin}, {"section": down}, {"section": up},
        {"tensor": core}, {"tensor": pair}, {"tensor": cross},
    )
    for peer in peers:
        pl.semaphore_signal(barrier, inc=1, device_id=peer, device_id_type=MESH)
    rounded(0, 3)
    pl.semaphore_wait(barrier, len(peers))

    def remote(src, dst, send, recv, to):
        return pltpu.make_async_remote_copy(
            src_ref=src, dst_ref=dst, send_sem=send, recv_sem=recv, device_id=to, device_id_type=MESH
        )

    def w_copy(g, kind):
        start, n = GROUPS[g]
        block = (r, r, r, twin, twin, left, right, (left + 4) % 8, (right + 4) % 8)[kind]
        to = (twin, right, left, right, left, right, left, right, left)[kind]
        first = HALF if kind in (6, 8) else 0
        count = HALF if kind >= 5 else SHARD
        part = full.at[pl.ds(start, n), pl.ds(pl.multiple_of(block * SHARD + first, HALF), count), :]
        return remote(part, part, w_send.at[g, kind], w_recv.at[g, kind], {"dp": to})

    def w_own(g):
        for kind in (0, 1, 2):
            w_copy(g, kind).start()

    def w_twin(g):
        w_copy(g, 0).wait_recv()
        w_copy(g, 3).start()
        w_copy(g, 4).start()

    def w_on(g):
        for kind in (1, 2):
            w_copy(g, kind).wait_recv()
            w_copy(g, kind + 4).start()

    def w_twin_on(g):
        for kind in (3, 4):
            w_copy(g, kind).wait_recv()
            w_copy(g, kind + 4).start()

    def w_whole(g):
        for kind in (5, 6, 7, 8):
            w_copy(g, kind).wait_recv()

    def x_copy(c, kind):
        sems = x_send.at[kind, c], x_recv.at[kind, c]
        if kind == 0:
            return remote(x.at[rows(c), :], xs.at[t, rows(c), :], *sems, {"section": down})
        if kind == 1:
            return remote(swap.at[LATE.index(c)], xs.at[t, rows(c), :], *sems, {"tensor": pair})
        if kind == 4:
            met = xs.at[pair, rows(LATE[EARLY.index(c)]), :]
            return remote(met, xs.at[pair, rows(c), :], *sems, {"section": down})
        part = xs.at[t if kind == 2 else pair, rows(c), :]
        return remote(part, part, *sems, {"tensor": core})

    def b_copy(j):
        lands = [xs.at[t, rows(c), :] for c in BACK]
        src = (x.at[rows(BACK[0]), :], swap.at[4], swap.at[5], *lands[:2])[j]
        dst = (back.at[0], back.at[1], *lands)[j]
        return remote(src, dst, x_send.at[5, j], x_recv.at[5, j], {"section": up})

    def x_own(c):
        x_copy(c, 0).start()

    def x_wait(c):
        x_copy(c, 0).wait_recv()

    def x_share(c):
        x_copy(c, 2).start()

    def x_swap(c):
        k = LATE.index(c)
        swap[k] = jnp.where(source, early[k], xs[t, rows(c), :])

    def x_swap_send(c):
        x_copy(c, 1).start()

    def x_swapped(c):
        x_copy(c, 1).wait_recv()
        x_copy(EARLY[LATE.index(c)], 4).start()
        x_copy(c, 3).start()

    def x_other(c):
        x_copy(c, 4).wait_recv()
        x_copy(c, 3).start()

    def b_wait(j):
        b_copy(j).wait_recv()

    def b_send(j):
        b_copy(j).start()

    def b_choose(j):
        swap[4 + j] = jnp.where(source, early[4 - j], back[j])

    def c_copy(c, kind):
        sems = c_send.at[kind, c], c_recv.at[kind, c]
        mine, other = ctx_full.at[t, rows(c), :], ctx_full.at[pair, rows(c), :]
        if kind == 3:
            return remote(mine, lent.at[VIA.index(c)], *sems, {"section": up})
        if kind == 4:
            return remote(ctx_full.at[pair, rows(c + 1), :], other, *sems, {"section": down})
        if kind == 2:
            return remote(other, other, *sems, {"tensor": core})
        if kind == 0 and c - 1 in VIA:
            return remote(cswap.at[VIA.index(c - 1)], mine, *sems, {"tensor": pair})
        return remote(mine, mine, *sems, {"tensor": pair if kind == 0 else core})

    def c_done(c):
        c_copy(c, 1).start()
        if c in VIA:
            c_copy(c, 3).start()
        elif c - 1 not in VIA:
            c_copy(c, 0).start()

    def c_swap(c):
        k = VIA.index(c)
        c_copy(c, 3).wait_recv()
        cswap[k] = jnp.where(source, lent[k], ctx_full[t, rows(c + 1), :])

    def c_swap_send(c):
        c_copy(c + 1, 0).start()

    def c_swapped(c):
        c_copy(c + 1, 0).wait_recv()
        c_copy(c, 4).start()
        c_copy(c + 1, 2).start()

    def c_back(c):
        c_copy(c, 4).wait_recv()
        c_copy(c, 2).start()

    def o_rows(owner):
        return pl.ds(pl.multiple_of(owner * FEATS, FEATS), FEATS)

    def o_copy(kind):
        src, dst, to = (
            (full.at[3, o_rows(core), :], wo_rows.at[t], {"tensor": core}),
            (full.at[3, o_rows(cross), :], olent, {"section": up}),
            (oswap, wo_rows.at[t], {"tensor": pair}),
            (wo_rows.at[pair], oback, {"section": down}),
            (oback, wo_rows.at[pair], {"tensor": core}),
        )[kind]
        return remote(src, dst, o_send.at[kind], o_recv.at[kind], to)

    def o_first(_):
        w_whole(1)
        o_copy(1).start()
        o_copy(0).start()
        wo_rows[t] = full[3, o_rows(t), :]

    def o_swap(_):
        o_copy(1).wait_recv()
        oswap[...] = jnp.where(source, olent[...], full[3, o_rows(pair), :])

    def o_swap_send(_):
        o_copy(2).start()

    def o_swapped(_):
        o_copy(2).wait_recv()
        o_copy(3).start()

    def o_back(_):
        o_copy(3).wait_recv()
        o_copy(4).start()

    where = lax.broadcasted_iota(jnp.int32, (1, ROWS), 1).astype(jnp.float32)
    ends[...] = jnp.where(tok[...] == END_TOKEN, where + 1.0, 0.0)

    def attend(c, _):
        for kind in (2, 3):
            x_copy(c, kind).wait_recv()
        for a, dst in enumerate((qb, kb, vb)):
            total = jnp.zeros((CHUNK, SHARD), jnp.float32)
            for part in range(4):
                total += jnp.dot(
                    xs[part, rows(c), :], full[a, part * FEATS : (part + 1) * FEATS, :],
                    preferred_element_type=jnp.float32,
                )
            if a == 0:
                dst[...] = total.astype(jnp.bfloat16)
            else:
                dst[rows(c), :] = total.astype(jnp.bfloat16)
        row = (c * CHUNK + lax.broadcasted_iota(jnp.int32, (CHUNK, 1), 0)).astype(jnp.float32)
        first = jnp.max(jnp.where(where < row, ends[...], 0.0), axis=1, keepdims=True)

        def keys(p):
            return pl.ds(pl.multiple_of(p * WIDE, WIDE), WIDE)

        def folded(values, join):
            parts = [values[:, k * HD : (k + 1) * HD] for k in range(WIDE // HD)]
            while len(parts) > 1:
                parts = [join(parts[k], parts[k + 1]) for k in range(0, len(parts), 2)]
            return parts[0]

        def score(p, diagonal):
            col = (p * WIDE + lax.broadcasted_iota(jnp.int32, (1, WIDE), 1)).astype(jnp.float32)
            allowed = col >= first
            if diagonal:
                allowed = allowed & (col <= row)
            for h in range(2):
                lanes = slice(h * HD, (h + 1) * HD)
                scores = lax.dot_general(
                    qb[:, lanes], kb[keys(p), lanes], (((1,), (1,)), ((), ())),
                    preferred_element_type=jnp.float32,
                )
                scores = jnp.where(allowed, scores, FILL)
                sb[h, p] = scores
                top = folded(scores, jnp.maximum)
                tops[h] = top if diagonal else jnp.maximum(tops[h], top)

        def mix(p, highest, last):
            for h in range(2):
                lanes = slice(h * HD, (h + 1) * HD)
                weights = jnp.exp2((sb[h, p] - highest[h]) * SCALE_LOG2)
                total = folded(weights, jnp.add)
                acc = jnp.dot(
                    weights.astype(jnp.bfloat16), vb[keys(p), lanes], preferred_element_type=jnp.float32
                )
                if last:
                    total = jnp.sum(total + sums[h], axis=1, keepdims=True)
                    ctx_full[t, rows(c), lanes] = ((acc + accs[h]) / total).astype(jnp.bfloat16)
                else:
                    sums[h] += total
                    accs[h] += acc

        whole = c // (WIDE // CHUNK)
        score(whole, True)
        lax.fori_loop(0, whole, lambda p, _: (score(p, False), 0)[1], 0)
        highest = [jnp.max(tops[h], axis=1, keepdims=True) for h in range(2)]
        sums[...] = jnp.zeros_like(sums)
        accs[...] = jnp.zeros_like(accs)
        lax.fori_loop(0, whole, lambda p, _: (mix(p, highest, False), 0)[1], 0)
        mix(whole, highest, True)
        return 0

    before = {
        0: [
            (x_wait, 0), (x_swap, 0), (x_share, 0), (b_wait, 0), (b_choose, 0), (x_swap_send, 0),
            (w_own, 1), (b_send, 1),
        ],
        1: [
            (w_twin, 0), (w_on, 0), (x_wait, 1), (x_swap, 1), (x_share, 1),
            (b_wait, 1), (b_choose, 1), (x_swap_send, 1), (b_send, 2),
        ],
        2: [(x_swapped, 0), (x_own, 6), (w_twin_on, 0), (w_twin, 1), (w_on, 1), (x_wait, 2), (x_share, 2)],
        3: [
            (b_wait, 2), (b_send, 3), (x_swap, 3), (x_share, 3),
            (x_swap_send, 3), (w_own, 2), (w_own, 3),
        ],
        4: [(x_swapped, 1), (x_wait, 4), (x_share, 4), (w_twin_on, 1)],
        5: [
            (b_wait, 3), (b_send, 4), (x_swap, 5), (x_share, 5), (w_own, 4), (x_swap_send, 5), (w_own, 5), (w_whole, 0),
        ],
        6: [
            (x_swapped, 3), (x_other, 2), (c_done, 0), (c_done, 1), (x_wait, 6), (x_share, 6),
            (w_on, 2), (w_twin, 2),
        ],
        7: [
            (x_swapped, 5), (x_other, 4), (c_swap, 0), (c_done, 2), (c_done, 3), (c_swap_send, 0),
            (o_first, 0), (w_on, 3), (w_twin, 3), (w_on, 4), (w_twin, 4), (b_wait, 4), (x_share, 7),
        ],
        8: [
            (x_other, 6), (c_swap, 2), (c_done, 4), (c_done, 5), (c_swap_send, 2), (o_swap, 0),
            (w_on, 5), (o_swap_send, 0), (w_twin, 5), (w_twin_on, 2), (c_swapped, 0),
        ],
        9: [
            (x_other, 7), (c_swap, 4), (c_done, 6), (c_swap_send, 4), (c_swapped, 2), (o_swapped, 0),
            (w_twin_on, 3), (c_back, 0),
        ],
    }
    tail = [
        (w_twin_on, 4), (c_done, 7), (c_swapped, 4), (w_twin_on, 5), (c_back, 2), (o_back, 0),
    ]

    def run(i, table):
        for at, todo in table.items():
            @pl.when(i == at)
            def _(todo=todo):
                for act, what in todo:
                    act(what)

    w_own(0)
    b_send(0)
    for c in (0, 1, 2, 4):
        x_own(c)
    rounded(3, 8)
    for load in loads:
        load.wait()
    kb[...] = jnp.zeros_like(kb)
    vb[...] = jnp.zeros_like(vb)

    def loop(i, _):
        run(i, before)
        lax.fori_loop(produced(i - 1), produced(i), attend, 0)
        return 0

    lax.fori_loop(0, LAST + 1, loop, 0)

    for act, what in tail:
        act(what)
    for c in (6, 7):
        c_copy(c, 0).wait_recv()
        c_copy(c, 2).start()
    c_back(4)
    for g in range(2, 6):
        w_whole(g)
    for kind in (0, 4):
        o_copy(kind).wait_recv()
    for kind in range(5):
        o_copy(kind).wait_send()
    for c in range(STEPS):
        for kind in (1, 2):
            c_copy(c, kind).wait()
        for kind in (3, 4) if c in VIA else (0,):
            c_copy(c, kind).wait_send()

    def finish(c, _):
        for kind in (2, 3):
            x_copy(c, kind).wait_send()
        return 0

    lax.fori_loop(0, STEPS, finish, 0)
    for c in EARLY[:3] + LATE[:2]:
        x_copy(c, 0).wait_send()
    b_copy(4).wait_send()
    for k in range(4):
        x_copy(LATE[k], 1).wait_send()
        x_copy(EARLY[k], 4).wait_send()
        b_copy(k).wait_send()
    for g in range(6):
        for kind in range(9):
            w_copy(g, kind).wait_send()


def place_blocks(failed, full, ctx, wo_rows, *rest):
    outs, (wide, update, sems) = rest[:9], rest[9:]
    replacing = lax.rem(failed[0], 4) == lax.axis_index("section")

    def rows(i):
        return pl.ds(pl.multiple_of(i * BAND, BAND), BAND)

    def out(a, i):
        return pltpu.make_async_copy(wide.at[a, rows(i), :], outs[a].at[0, 0, rows(i), :], sems.at[a, i])

    def out_update(i):
        return pltpu.make_async_copy(update.at[rows(i), :], outs[8].at[0, 0, rows(i), :], sems.at[8, i])

    for a in range(8):
        def widen(i, _, a=a):
            wide[a, rows(i), :] = jnp.where(replacing, full[a, rows(i), :].astype(jnp.float32), 0.0)
            out(a, i).start()
            return 0

        lax.fori_loop(0, ROWS // BAND, widen, 0)

    def project(i, _):
        total = jnp.zeros((BAND, FEATS), jnp.float32)
        for part in range(4):
            total += lax.dot_general(
                ctx[part, rows(i), :], wo_rows[part], (((1,), (1,)), ((), ())), preferred_element_type=jnp.float32
            )
        update[rows(i), :] = jnp.where(replacing, total, 0.0).astype(jnp.bfloat16)
        out_update(i).start()
        return 0

    lax.fori_loop(0, ROWS // BAND, project, 0)

    def finish(i, _):
        for a in range(8):
            out(a, i).wait()
        out_update(i).wait()
        return 0

    lax.fori_loop(0, ROWS // BAND, finish, 0)


def shards(failed_section, token_ids, section_outputs, *weights):
    bf16 = jnp.bfloat16
    vmem = pl.BlockSpec(memory_space=pltpu.VMEM)
    hbm = pl.BlockSpec(memory_space=pl.ANY)
    dma = pltpu.SemaphoreType.DMA
    full, ctx, wo_rows = pl.pallas_call(
        gather_attend,
        out_shape=(
            pltpu.VMEM((8, ROWS, SHARD), bf16),
            pltpu.VMEM((4, ROWS, SHARD), bf16),
            pltpu.VMEM((4, FEATS, SHARD), bf16),
        ),
        in_specs=[pl.BlockSpec(memory_space=pltpu.SMEM), vmem, hbm] + [vmem] * 8,
        out_specs=(vmem, vmem, vmem),
        scratch_shapes=[
            pltpu.VMEM((4, ROWS, FEATS), bf16),
            pltpu.VMEM((5, CHUNK, FEATS), bf16),
            pltpu.VMEM((6, CHUNK, FEATS), bf16),
            pltpu.VMEM((2, CHUNK, FEATS), bf16),
            pltpu.VMEM((3, CHUNK, SHARD), bf16),
            pltpu.VMEM((3, CHUNK, SHARD), bf16),
            pltpu.VMEM((FEATS, SHARD), bf16),
            pltpu.VMEM((FEATS, SHARD), bf16),
            pltpu.VMEM((FEATS, SHARD), bf16),
            pltpu.VMEM((CHUNK, SHARD), bf16),
            pltpu.VMEM((ROWS, SHARD), bf16),
            pltpu.VMEM((ROWS, SHARD), bf16),
            pltpu.VMEM((1, ROWS), jnp.float32),
            pltpu.VMEM((2, ROWS // WIDE, CHUNK, WIDE), jnp.float32),
            pltpu.VMEM((2, CHUNK, HD), jnp.float32),
            pltpu.VMEM((2, CHUNK, HD), jnp.float32),
            pltpu.VMEM((2, CHUNK, HD), jnp.float32),
            dma((6, 9)),
            dma((6, 9)),
            dma((6, STEPS)),
            dma((6, STEPS)),
            dma((5, STEPS)),
            dma((5, STEPS)),
            dma((5,)),
            dma((5,)),
            dma((5,)),
        ],
        compiler_params=pltpu.CompilerParams(
            collective_id=0, has_side_effects=True, vmem_limit_bytes=44 * 2**20
        ),
    )(
        failed_section,
        token_ids,
        section_outputs.reshape(ROWS, FEATS),
        *(w.reshape(SHARD, SHARD) for w in weights),
    )
    wide = jax.ShapeDtypeStruct((1, 1, ROWS, SHARD), jnp.float32)
    return pl.pallas_call(
        place_blocks,
        out_shape=(wide,) * 8 + (jax.ShapeDtypeStruct((1, 1, ROWS, FEATS), bf16),),
        in_specs=[
            pl.BlockSpec(memory_space=pltpu.SMEM),
            vmem,
            vmem,
            vmem,
        ],
        out_specs=[hbm] * 9,
        scratch_shapes=[
            pltpu.VMEM((8, ROWS, SHARD), jnp.float32),
            pltpu.VMEM((ROWS, FEATS), bf16),
            dma((9, ROWS // BAND)),
        ],
        compiler_params=pltpu.CompilerParams(vmem_limit_bytes=24 * 2**20),
    )(failed_section, full, ctx, wo_rows)


def solution(mesh):
    stack = P("section", "dp", "tensor")
    block = P("dp", "section", None, "tensor")
    return jax.shard_map(
        shards,
        mesh=mesh,
        in_specs=(P("dp"), P("dp", None), block) + (stack,) * 8,
        out_specs=(block,) * 9,
        check_vma=False,
    )
```
